256 devices in a mesh: rows: 32 (over y, x, core), cols: 8 (over z).
Axes of the slice: x: 4, y: 4, z: 8, core: 2. Of those that a mesh axis runs over, the one named last changes fastest.
Arguments:
- one_query: float32 [8192, 8192], P('rows', 'cols'), may hold values from -0.125 to 0.125
- other_query: float32 [8192, 8192], P('rows', 'cols'), may hold values from -0.0625 to 0.0625
- one_key: float32 [8192, 512], P('rows', 'cols'), may hold values from -0.125 to 0.125
- other_key: float32 [8192, 512], P('rows', 'cols'), may hold values from -0.0625 to 0.0625
- one_value: float32 [8192, 512], P('rows', 'cols'), may hold values from -0.125 to 0.125
- other_value: float32 [8192, 512], P('rows', 'cols'), may hold values from -0.0625 to 0.0625
- mix_share: float32 [8192], P('rows'), may hold values from 0.2 to 0.8
- norm_gain: float32 [8192], P('rows'), may hold values from 0.25 to 1.75
Outputs:
- serve_query: bfloat16 [8192, 8192], P(None, 'cols')
- serve_key: bfloat16 [8192, 512], P(None, 'cols')
- serve_value: bfloat16 [8192, 512], P(None, 'cols')
- scale_query: float32 [8192], P('cols')
- scale_key: float32 [512], P('cols')
- scale_value: float32 [512], P('cols')
The draws below stay inside these ranges and needn't reach their ends.
All inputs are finite; a program needn't handle non-finite values. Where the reference program divides by a largest or mean magnitude, that divisor is 1e-20 or more.
Results may differ from the reference program's by a relative error of at most 0.001.
Values may be sent and summed in bfloat16 or wider, within the bound.
A program may use at most 128 MiB of HBM per device.

```python
import jax
import jax.numpy as jnp

D_MODEL = 8192
Q_DIM = 8192
KV_DIM = 512


def strengthened(drawn, stream_key, source, target, parts, factor):
    owner, partner = [(jnp.arange(drawn.shape[dim]) // (drawn.shape[dim] // parts)).reshape([-1 if axis == dim else 1 for axis in range(drawn.ndim)]) for dim in (source, target)]
    chosen = jax.random.permutation(stream_key, parts)[partner]
    strong = (owner == chosen) | (owner == (partner + parts // 2) % parts)
    return jnp.where(strong, factor * drawn, drawn)


def block_levels(own_key, extent, cuts, low, high):
    level, own = 1.0, jax.random.fold_in(own_key, 6)
    for axis_at, parts in cuts:
        steps = jnp.exp(jax.random.uniform(jax.random.fold_in(own, axis_at), (parts,), jnp.float32, low / len(cuts), high / len(cuts)))
        level = level * jnp.repeat(steps, extent[axis_at] // parts).reshape([-1 if axis == axis_at else 1 for axis in range(len(extent))])
    return level


def gaussian(own_key, extent, width, reach, shards=(), dtype=jnp.bfloat16):
    drawn = width * jax.random.normal(own_key, extent, jnp.float32)
    if shards:
        drawn = drawn * block_levels(own_key, extent, shards, -0.22, 0.18)
    return jnp.clip(drawn, -reach, reach).astype(dtype)


def gaussian_with(own_key, dims, deviation, reach, cuts, heavy, dtype=jnp.bfloat16):
    drawn = deviation * jax.random.normal(own_key, dims, jnp.float32)
    if cuts:
        drawn = drawn * block_levels(own_key, dims, cuts, -0.22, 0.18)
    return jnp.clip(strengthened(drawn, jax.random.fold_in(own_key, 3), *heavy), -reach, reach).astype(dtype)


def setup_inputs(seed: int = 0) -> dict:
    streams_of = jax.random.split(jax.random.key(seed), 9)
    one_query = gaussian_with(streams_of[0], (D_MODEL, Q_DIM), D_MODEL ** -0.5, 0.125, ((0, 32), (1, 8)), (0, 1, 32, 2.75), jnp.float32)
    other_query = gaussian(streams_of[1], (D_MODEL, Q_DIM), D_MODEL ** -0.5, 0.0625, ((0, 32), (1, 8)), jnp.float32)
    one_key = gaussian_with(streams_of[2], (D_MODEL, KV_DIM), D_MODEL ** -0.5, 0.125, ((0, 32), (1, 8)), (0, 1, 32, 2.75), jnp.float32)
    other_key = gaussian(streams_of[3], (D_MODEL, KV_DIM), D_MODEL ** -0.5, 0.0625, ((0, 32), (1, 8)), jnp.float32)
    one_value = gaussian_with(streams_of[4], (D_MODEL, KV_DIM), D_MODEL ** -0.5, 0.125, ((0, 32), (1, 8)), (0, 1, 32, 2.75), jnp.float32)
    other_value = gaussian(streams_of[5], (D_MODEL, KV_DIM), D_MODEL ** -0.5, 0.0625, ((0, 32), (1, 8)), jnp.float32)
    mix_share = jnp.clip(0.2 + 0.6 * jax.random.uniform(streams_of[6], (D_MODEL,), jnp.float32) ** block_levels(streams_of[6], (D_MODEL,), ((0, 32),), -0.2, 0.2), 0.2, 0.8)
    norm_gain = jnp.clip(1.0 + 0.15 * jax.random.normal(streams_of[7], (D_MODEL,), jnp.float32), 0.25, 1.75)
    return dict(one_query=one_query, other_query=other_query, one_key=one_key, other_key=other_key, one_value=one_value, other_value=other_value, mix_share=mix_share, norm_gain=norm_gain)


def reference(one_query, other_query, one_key, other_key, one_value, other_value, mix_share, norm_gain):
    fresh_query = mix_share[:, None] * one_query + (1.0 - mix_share[:, None]) * other_query
    fresh_key = mix_share[:, None] * one_key + (1.0 - mix_share[:, None]) * other_key
    fresh_value = mix_share[:, None] * one_value + (1.0 - mix_share[:, None]) * other_value
    fresh_gained_query = fresh_query * norm_gain[:, None]
    fresh_gained_key = fresh_key * norm_gain[:, None]
    fresh_gained_value = fresh_value * norm_gain[:, None]
    scale_query = jnp.sum(jnp.abs(fresh_gained_query), axis=0) / D_MODEL
    serve_query = (fresh_gained_query / scale_query).astype(jnp.bfloat16)
    scale_key = jnp.sum(jnp.abs(fresh_gained_key), axis=0) / D_MODEL
    serve_key = (fresh_gained_key / scale_key).astype(jnp.bfloat16)
    scale_value = jnp.sum(jnp.abs(fresh_gained_value), axis=0) / D_MODEL
    serve_value = (fresh_gained_value / scale_value).astype(jnp.bfloat16)
    return serve_query, serve_key, serve_value, scale_query, scale_key, scale_value
```

```python
import functools
import math

import jax
import jax.numpy as jnp
from jax import lax
from jax.experimental import pallas as pl
from jax.experimental.pallas import tpu as pltpu
from jax.sharding import PartitionSpec as P

MESH = pl.DeviceIdType.MESH
CHUNKS = 2
SLABS = 4
STEP_ROWS = 32


def chip_at(cycle, place, side):
    major = lax.div(place, side)
    minor = lax.rem(place - major + side, side)
    y, x = (minor, major) if cycle == 0 else (major, minor)
    return y * side + x


def place_of(cycle, chip, side):
    y, x = lax.div(chip, side), lax.rem(chip, side)
    major, minor = (x, y) if cycle == 0 else (y, x)
    return major * side + lax.rem(minor + major, side)


def gather_kernel(
    ranks, d_model,
    mix_hbm, gain_hbm, oq, tq, ok, tk, ov, tv,
    sq, sk, sv, cq, ck, cv,
    mix, gain, one, other, one_kv, other_kv, col_a, col_b, sums,
    coef_sem, q_sem, kv_sem, stat_send, stat_recv, ring_send, ring_recv,
    own_send, own_recv, twin_send, twin_recv,
):
    me = lax.axis_index("rows")
    chips = ranks // 2
    side = math.isqrt(chips)
    steps = chips // 2
    chip, core = lax.div(me, 2), lax.rem(me, 2)
    twin = chip * 2 + 1 - core
    rows, q_cols = oq.shape
    kv_cols = ok.shape[0]
    half = rows // 2
    chunk = half // CHUNKS
    slab = rows // SLABS
    tiles = q_cols // 128

    loads = []
    for n, (source, held) in enumerate(((mix_hbm, mix), (gain_hbm, gain))):
        copy = pltpu.make_async_copy(source, held, coef_sem.at[n])
        copy.start()
        loads.append(copy)
    q_loads = []
    for s in range(SLABS):
        r = pl.ds(s * slab, slab)
        pair = []
        for n, (source, held) in enumerate(((oq, one), (tq, other))):
            copy = pltpu.make_async_copy(source.at[r], held.at[r], q_sem.at[n, s])
            copy.start()
            pair.append(copy)
        q_loads.append(pair)
    kv_loads = []
    for n, (source, held) in enumerate(
        ((ok, one_kv.at[pl.ds(0, kv_cols)]), (tk, other_kv.at[pl.ds(0, kv_cols)]),
         (ov, one_kv.at[pl.ds(kv_cols, kv_cols)]), (tv, other_kv.at[pl.ds(kv_cols, kv_cols)]))
    ):
        copy = pltpu.make_async_copy(source, held, kv_sem.at[n])
        copy.start()
        kv_loads.append(copy)

    barrier = pltpu.get_barrier_semaphore()
    for shift in range(1, ranks):
        pl.semaphore_signal(
            barrier, inc=1, device_id={"rows": lax.rem(me + shift, ranks)}, device_id_type=MESH
        )

    for copy in loads:
        copy.wait()
    a_row = gain[...] * mix[...]
    b_row = gain[...] * (1.0 - mix[...])
    for c in range(0, rows, 128):
        col_a[pl.ds(c, 128), :] = jnp.broadcast_to(a_row[:, c:c + 128], (128, 128)).T
        col_b[pl.ds(c, 128), :] = jnp.broadcast_to(b_row[:, c:c + 128], (128, 128)).T

    accs = tuple(jnp.zeros((8, 128), jnp.float32) for _ in range(tiles))
    for s in range(SLABS):
        for copy in q_loads[s]:
            copy.wait()

        def body(i, accs):
            r = pl.ds(pl.multiple_of(s * slab + i * STEP_ROWS, STEP_ROWS), STEP_ROWS)
            a, b = col_a[r, :], col_b[r, :]
            new = []
            for j, acc in enumerate(accs):
                c = pl.ds(j * 128, 128)
                f = a * one[r, c] + b * other[r, c]
                one[r, c] = f
                new.append(acc + jnp.sum(jnp.abs(f).reshape(STEP_ROWS // 8, 8, 128), axis=0))
            return tuple(new)

        accs = lax.fori_loop(0, slab // STEP_ROWS, body, accs)
    for j, acc in enumerate(accs):
        sums[me, pl.ds(j, 1), :] = jnp.sum(acc, axis=0, keepdims=True)
    for copy in kv_loads:
        copy.wait()
    f = a_row * one_kv[...] + b_row * other_kv[...]
    one_kv[...] = f
    sizes = jnp.abs(f)
    size = sizes[:, 0:128]
    for c in range(128, rows, 128):
        size = size + sizes[:, c:c + 128]
    sums[me, pl.ds(tiles, 1), :] = jnp.sum(size.T, axis=0, keepdims=True)

    def remote(src, dst, send, recv, device):
        copy = pltpu.make_async_remote_copy(
            src_ref=src, dst_ref=dst, send_sem=send, recv_sem=recv,
            device_id={"rows": device}, device_id_type=MESH,
        )
        copy.start()
        return copy

    pl.semaphore_wait(barrier, ranks - 1)
    stats = []
    for shift in range(1, ranks):
        place = sums.at[me]
        stats.append(remote(
            place, place, stat_send.at[shift], stat_recv.at[shift], lax.rem(me + shift, ranks)
        ))

    spots = [place_of(c, chip, side) for c in range(2)]
    aims = {}
    for c in range(2):
        aims[c, 0] = chip_at(c, lax.rem(spots[c] + 1, chips), side) * 2 + core
        aims[c, 1] = chip_at(c, lax.rem(spots[c] + chips - 1, chips), side) * 2 + core

    for copy in stats:
        copy.wait_recv()
    total = sums[0, 0:tiles + 1, :]
    for owner in range(1, ranks):
        total = total + sums[owner, 0:tiles + 1, :]
    scale = total / d_model
    inverse = 1.0 / scale

    def piece(c, dev, n, way=None):
        if n < CHUNKS:
            at = pl.multiple_of(dev * rows + c * half + n * chunk, chunk)
            return sq.at[pl.ds(at, chunk)]
        ref = (sk, sv)[c]
        at = pl.ds(pl.multiple_of(dev * rows, rows), rows)
        if way is None:
            return ref.at[:, at]
        return ref.at[pl.ds(way * (kv_cols // 2), kv_cols // 2), at]

    def parts(step, way):
        if step < steps:
            return list(range(CHUNKS + 1))
        return list(range(way * CHUNKS // 2, (way + 1) * CHUNKS // 2)) + [CHUNKS]

    ring = {}
    twins = {}

    def launch(c, way, step, n, dev):
        spot = piece(c, dev, n, way if step == steps else None)
        ring[c, way, step, n] = remote(
            spot, spot, ring_send.at[c, way, step - 1, n], ring_recv.at[c, way, step - 1, n],
            aims[c, way],
        )

    for n in range(CHUNKS):
        for c in range(2):
            def body(i, carry, c=c, n=n):
                first = c * half + n * chunk + i * STEP_ROWS
                r = pl.ds(pl.multiple_of(first, STEP_ROWS), STEP_ROWS)
                to = pl.ds(pl.multiple_of(me * rows + first, STEP_ROWS), STEP_ROWS)
                for j in range(tiles):
                    col = pl.ds(j * 128, 128)
                    sq[to, col] = (one[r, col] * inverse[j:j + 1, :]).astype(jnp.bfloat16)
                return carry

            lax.fori_loop(0, chunk // STEP_ROWS, body, 0)
            for way in range(2):
                launch(c, way, 1, n, me)
    flip = jnp.broadcast_to(inverse[tiles:tiles + 1, :], (128, 128)).T
    own = pl.multiple_of(me * rows, rows)
    for c, ref in enumerate((sk, sv)):
        r = pl.ds(c * kv_cols, kv_cols)
        for col in range(0, rows, 128):
            ref[:, pl.ds(pl.multiple_of(own + col, 128), 128)] = (
                one_kv[r, pl.ds(col, 128)] * flip[c * kv_cols:(c + 1) * kv_cols, :]
            ).astype(jnp.bfloat16)
        for way in range(2):
            launch(c, way, 1, CHUNKS, me)
    for c in range(2):
        for n in range(CHUNKS + 1):
            spot = piece(c, me, n)
            twins[c, n] = remote(spot, spot, own_send.at[c, n], own_recv.at[c, n], twin)

    for j in range(tiles):
        cq[:, pl.ds(j * 128, 128)] = scale[j:j + 1, :]
    ck[...] = scale[tiles:tiles + 1, 0:kv_cols]
    cv[...] = scale[tiles:tiles + 1, kv_cols:2 * kv_cols]

    for step in range(1, steps + 1):
        devs = {}
        for c in range(2):
            devs[c, 0] = chip_at(c, lax.rem(spots[c] + chips - step, chips), side) * 2 + core
            devs[c, 1] = chip_at(c, lax.rem(spots[c] + step, chips), side) * 2 + core
        for n in range(CHUNKS + 1):
            for c in range(2):
                for way in range(2):
                    if n not in parts(step, way):
                        continue
                    ring[c, way, step, n].wait_recv()
                    if step < steps and n in parts(step + 1, way):
                        launch(c, way, step + 1, n, devs[c, way])
                    spot = piece(c, devs[c, way], n, way if step == steps else None)
                    twins[c, way, step, n] = remote(
                        spot, spot, twin_send.at[c, way, step - 1, n],
                        twin_recv.at[c, way, step - 1, n], twin,
                    )
    for copy in stats:
        copy.wait_send()
    for copy in ring.values():
        copy.wait_send()
    for copy in twins.values():
        copy.wait()


def write_kernel(sq, sk, sv, cq, ck, cv, oq, ok, ov, dq, dk, dv, q_sem, sem):
    count = q_sem.shape[0]
    rows = sq.shape[0] // count
    copies = []
    for n in range(count):
        r = pl.ds(n * rows, rows)
        copies.append(pltpu.make_async_copy(sq.at[r], oq.at[r], q_sem.at[n]))
    for n, (source, out) in enumerate(((sk, ok), (sv, ov), (cq, dq), (ck, dk), (cv, dv))):
        copies.append(pltpu.make_async_copy(source, out, sem.at[n]))
    for copy in copies:
        copy.start()
    for copy in copies:
        copy.wait()


def local(ranks, d_model, one_query, other_query, one_key, other_key, one_value, other_value, mix_share, norm_gain):
    rows, q_cols = one_query.shape
    kv_cols = one_key.shape[1]
    whole = ranks * rows
    steps = ranks // 4
    vmem = pl.BlockSpec(memory_space=pltpu.VMEM)
    hbm = pl.BlockSpec(memory_space=pltpu.HBM)
    dma = pltpu.SemaphoreType.DMA
    f32, bf16 = jnp.float32, jnp.bfloat16
    shapes = (
        jax.ShapeDtypeStruct((whole, q_cols), bf16),
        jax.ShapeDtypeStruct((kv_cols, whole), bf16),
        jax.ShapeDtypeStruct((kv_cols, whole), bf16),
        jax.ShapeDtypeStruct((1, q_cols), f32),
        jax.ShapeDtypeStruct((1, kv_cols), f32),
        jax.ShapeDtypeStruct((1, kv_cols), f32),
    )
    pieces = CHUNKS + 1
    landed = pl.pallas_call(
        functools.partial(gather_kernel, ranks, d_model),
        out_shape=tuple(pltpu.VMEM(x.shape, x.dtype) for x in shapes),
        in_specs=[hbm] * 8,
        out_specs=(vmem,) * 6,
        scratch_shapes=[
            pltpu.VMEM((1, rows), f32),
            pltpu.VMEM((1, rows), f32),
            pltpu.VMEM((rows, q_cols), f32),
            pltpu.VMEM((rows, q_cols), f32),
            pltpu.VMEM((2 * kv_cols, rows), f32),
            pltpu.VMEM((2 * kv_cols, rows), f32),
            pltpu.VMEM((rows, 128), f32),
            pltpu.VMEM((rows, 128), f32),
            pltpu.VMEM((ranks, 16, 128), f32),
            dma((2,)),
            dma((2, SLABS)),
            dma((4,)),
            dma((ranks,)),
            dma((ranks,)),
            dma((2, 2, steps, pieces)),
            dma((2, 2, steps, pieces)),
            dma((2, pieces)),
            dma((2, pieces)),
            dma((2, 2, steps, pieces)),
            dma((2, 2, steps, pieces)),
        ],
        compiler_params=pltpu.CompilerParams(
            collective_id=0, has_side_effects=True, vmem_limit_bytes=VMEM_A
        ),
    )(*(
        pltpu.with_memory_space_constraint(x, pltpu.HBM)
        for x in (
            mix_share.reshape(1, rows), norm_gain.reshape(1, rows), one_query, other_query,
            one_key.T, other_key.T, one_value.T, other_value.T,
        )
    ))
    out = pl.pallas_call(
        write_kernel,
        out_shape=shapes,
        in_specs=[vmem] * 6,
        out_specs=(hbm,) * 6,
        scratch_shapes=[dma((8,)), dma((5,))],
        compiler_params=pltpu.CompilerParams(vmem_limit_bytes=VMEM_B),
    )(*landed)
    sq, sk, sv, cq, ck, cv = out
    return sq, sk.T, sv.T, cq[0], ck[0], cv[0]


VMEM_A = 10 * 1024 * 1024
VMEM_B = 2 * 1024 * 1024


def solution(mesh):
    def body(one_query, *rest):
        ranks = mesh.shape["rows"]
        return local(ranks, ranks * one_query.shape[0], one_query, *rest)

    return jax.shard_map(
        body,
        mesh=mesh,
        in_specs=(P("rows", "cols"),) * 6 + (P("rows"),) * 2,
        out_specs=(P(None, "cols"),) * 3 + (P("cols"),) * 3,
        check_vma=False,
    )
```

```python
import functools
import math

import jax
import jax.numpy as jnp
from jax import lax
from jax.experimental import pallas as pl
from jax.experimental.pallas import tpu as pltpu
from jax.sharding import PartitionSpec as P

MESH = pl.DeviceIdType.MESH
CHUNKS = 2
SLABS = 4
STEP_ROWS = 32


def chip_at(cycle, place, side):
    major = lax.div(place, side)
    minor = lax.rem(place - major + side, side)
    y, x = (minor, major) if cycle == 0 else (major, minor)
    return y * side + x


def place_of(cycle, chip, side):
    y, x = lax.div(chip, side), lax.rem(chip, side)
    major, minor = (x, y) if cycle == 0 else (y, x)
    return major * side + lax.rem(minor + major, side)


def gather_kernel(
    ranks, d_model,
    mix_hbm, gain_hbm, oq, tq, ok, tk, ov, tv,
    sq, sk, sv, cq, ck, cv,
    coefs, q_in, kv_in, col_a, col_b, sums,
    load_sem, stat_sem, ring_sem, twin_sem, ring_recv,
):
    me = lax.axis_index("rows")
    chips = ranks // 2
    side = math.isqrt(chips)
    steps = chips // 2
    chip, core = lax.div(me, 2), lax.rem(me, 2)
    twin = chip * 2 + 1 - core
    rows, q_cols = oq.shape
    kv_cols = ok.shape[0]
    half = rows // 2
    chunk = half // CHUNKS
    slab = rows // SLABS
    tiles = q_cols // 128
    one, one_kv = q_in.at[0], kv_in.at[0]

    barrier = pltpu.get_barrier_semaphore()
    for shift in range(1, ranks):
        pl.semaphore_signal(
            barrier, inc=1, device_id={"rows": lax.rem(me + shift, ranks)}, device_id_type=MESH
        )

    def load(source, held, sem):
        pltpu.make_async_copy(source, held, sem).start()

    def settle(ref, sem):
        pltpu.make_async_copy(ref, ref, sem).wait()

    load(mix_hbm, coefs.at[0], load_sem.at[0])
    load(gain_hbm, coefs.at[1], load_sem.at[0])
    for s in range(SLABS):
        r = pl.ds(s * slab, slab)
        for n, source in enumerate((oq, tq)):
            load(source.at[r], q_in.at[n, r], load_sem.at[2 + s])
    for n, source in enumerate((ok, tk, ov, tv)):
        load(source, kv_in.at[n % 2, pl.ds(n // 2 * kv_cols, kv_cols)], load_sem.at[1])

    settle(coefs, load_sem.at[0])
    a_row = coefs[1] * coefs[0]
    b_row = coefs[1] * (1.0 - coefs[0])
    for c in range(0, rows, 128):
        col_a[pl.ds(c, 128), :] = jnp.broadcast_to(a_row[:, c:c + 128], (128, 128)).T
        col_b[pl.ds(c, 128), :] = jnp.broadcast_to(b_row[:, c:c + 128], (128, 128)).T

    accs = tuple(jnp.zeros((8, 128), jnp.float32) for _ in range(tiles))
    for s in range(SLABS):
        settle(q_in.at[:, pl.ds(s * slab, slab)], load_sem.at[2 + s])

        def body(i, accs):
            r = pl.ds(pl.multiple_of(s * slab + i * STEP_ROWS, STEP_ROWS), STEP_ROWS)
            a, b = col_a[r, :], col_b[r, :]
            new = []
            for j, acc in enumerate(accs):
                c = pl.ds(j * 128, 128)
                f = a * q_in[0, r, c] + b * q_in[1, r, c]
                one[r, c] = f
                new.append(acc + jnp.sum(jnp.abs(f).reshape(STEP_ROWS // 8, 8, 128), axis=0))
            return tuple(new)

        accs = lax.fori_loop(0, slab // STEP_ROWS, body, accs)
    for j, acc in enumerate(accs):
        sums[me, pl.ds(j, 1), :] = jnp.sum(acc, axis=0, keepdims=True)
    settle(kv_in, load_sem.at[1])
    f = a_row * kv_in[0] + b_row * kv_in[1]
    one_kv[...] = f
    sizes = jnp.abs(f)
    size = sizes[:, 0:128]
    for c in range(128, rows, 128):
        size = size + sizes[:, c:c + 128]
    sums[me, pl.ds(tiles, 1), :] = jnp.sum(size.T, axis=0, keepdims=True)

    def remote(src, dst, send, recv, device):
        pltpu.make_async_remote_copy(
            src_ref=src, dst_ref=dst, send_sem=send, recv_sem=recv,
            device_id={"rows": device}, device_id_type=MESH,
        ).start()

    pl.semaphore_wait(barrier, ranks - 1)
    place = sums.at[me, pl.ds(0, tiles + 1)]
    for shift in range(1, ranks):
        remote(place, place, stat_sem.at[0], stat_sem.at[1], lax.rem(me + shift, ranks))

    spots = [place_of(c, chip, side) for c in range(2)]
    aims = {}
    for c in range(2):
        aims[c, 0] = chip_at(c, lax.rem(spots[c] + 1, chips), side) * 2 + core
        aims[c, 1] = chip_at(c, lax.rem(spots[c] + chips - 1, chips), side) * 2 + core

    peers = sums.at[pl.ds(0, ranks - 1), pl.ds(0, tiles + 1)]
    settle(peers, stat_sem.at[1])
    total = sums[0, 0:tiles + 1, :]
    for owner in range(1, ranks):
        total = total + sums[owner, 0:tiles + 1, :]
    scale = total / d_model
    inverse = 1.0 / scale

    def pieces(step, way):
        if step < steps:
            order = range(CHUNKS) if way == 0 else range(CHUNKS - 1, -1, -1)
            return [(n * chunk, chunk, 2 if at == 0 else None) for at, n in enumerate(order)]
        part = half // 4
        firsts = (0, part) if way == 0 else (half - part, half - 2 * part)
        return [(first, part, way if at == 0 else None) for at, first in enumerate(firsts)]

    def refs(c, dev, item):
        first, count, share = item
        at = pl.multiple_of(dev * rows + c * half + first, 32)
        out = [sq.at[pl.ds(at, count)]]
        if share is not None:
            at = pl.ds(pl.multiple_of(dev * rows, rows), rows)
            ref = (sk, sv)[c]
            if share < 2:
                ref = ref.at[pl.ds(share * (kv_cols // 2), kv_cols // 2)]
            out.append(ref.at[:, at])
        return out

    def ring(c, way, step, at, dev):
        for ref in refs(c, dev, pieces(step, way)[at]):
            remote(ref, ref, ring_sem.at[0], ring_recv.at[c, way, step - 1, at], aims[c, way])

    def settle_ring(c, way, step, at):
        first, count, share = pieces(step, way)[at]
        extra = 0 if share is None else kv_cols * rows // q_cols // (1 if share == 2 else 2)
        settle(sq.at[pl.ds(0, count + extra)], ring_recv.at[c, way, step - 1, at])

    def pass_on(c, dev, item):
        for ref in refs(c, dev, item):
            remote(ref, ref, twin_sem.at[0], twin_sem.at[1], twin)

    flip = jnp.broadcast_to(inverse[tiles:tiles + 1, :], (128, 128)).T
    own = pl.multiple_of(me * rows, rows)
    for c, ref in enumerate((sk, sv)):
        r = pl.ds(c * kv_cols, kv_cols)
        for col in range(0, rows, 128):
            ref[:, pl.ds(pl.multiple_of(own + col, 128), 128)] = (
                one_kv[r, pl.ds(col, 128)] * flip[c * kv_cols:(c + 1) * kv_cols, :]
            ).astype(jnp.bfloat16)
    made = set()
    sent = set()
    for n in [k for pair in zip(range(CHUNKS), range(CHUNKS - 1, -1, -1)) for k in pair]:
        if n in made:
            continue
        made.add(n)
        for c in range(2):
            def body(i, carry, c=c, n=n):
                first = c * half + n * chunk + i * STEP_ROWS
                r = pl.ds(pl.multiple_of(first, STEP_ROWS), STEP_ROWS)
                to = pl.ds(pl.multiple_of(me * rows + first, STEP_ROWS), STEP_ROWS)
                for j in range(tiles):
                    col = pl.ds(j * 128, 128)
                    sq[to, col] = (one[r, col] * inverse[j:j + 1, :]).astype(jnp.bfloat16)
                return carry

            lax.fori_loop(0, chunk // STEP_ROWS, body, 0)
        for at in range(CHUNKS):
            for c in range(2):
                for way in range(2):
                    ready = {(k[0] // chunk) for k in pieces(1, way)[:at + 1]}
                    if ready <= made and (c, way, at) not in sent:
                        sent.add((c, way, at))
                        ring(c, way, 1, at, me)
    for c in range(2):
        pass_on(c, me, (0, half, 2))

    for j in range(tiles):
        cq[:, pl.ds(j * 128, 128)] = scale[j:j + 1, :]
    ck[...] = scale[tiles:tiles + 1, 0:kv_cols]
    cv[...] = scale[tiles:tiles + 1, kv_cols:2 * kv_cols]

    for step in range(1, steps + 1):
        devs = {}
        for c in range(2):
            devs[c, 0] = chip_at(c, lax.rem(spots[c] + chips - step, chips), side) * 2 + core
            devs[c, 1] = chip_at(c, lax.rem(spots[c] + step, chips), side) * 2 + core
        for at in range(len(pieces(step, 0))):
            for c in range(2):
                for way in range(2):
                    settle_ring(c, way, step, at)
                    item = pieces(step, way)[at]
                    if step < steps:
                        for later, nxt in enumerate(pieces(step + 1, way)):
                            if item[0] <= nxt[0] < item[0] + item[1]:
                                ring(c, way, step + 1, later, devs[c, way])
                    pass_on(c, devs[c, way], item)
    settle(peers, stat_sem.at[0])
    share = half + kv_cols * rows // q_cols
    settle(sq.at[pl.ds(0, 2 * (chips - 1) * share)], ring_sem.at[0])
    settle(sq.at[pl.ds(0, 2 * chips * share)], twin_sem.at[0])
    settle(sq.at[pl.ds(0, 2 * chips * share)], twin_sem.at[1])


def write_kernel(sq, sk, sv, cq, ck, cv, oq, ok, ov, dq, dk, dv, q_sem, sem):
    count = q_sem.shape[0]
    rows = sq.shape[0] // count
    copies = []
    for n in range(count):
        r = pl.ds(n * rows, rows)
        copies.append(pltpu.make_async_copy(sq.at[r], oq.at[r], q_sem.at[n]))
    for n, (source, out) in enumerate(((sk, ok), (sv, ov), (cq, dq), (ck, dk), (cv, dv))):
        copies.append(pltpu.make_async_copy(source, out, sem.at[n]))
    for copy in copies:
        copy.start()
    for copy in copies:
        copy.wait()


def local(ranks, d_model, one_query, other_query, one_key, other_key, one_value, other_value, mix_share, norm_gain):
    rows, q_cols = one_query.shape
    kv_cols = one_key.shape[1]
    whole = ranks * rows
    steps = ranks // 4
    vmem = pl.BlockSpec(memory_space=pltpu.VMEM)
    hbm = pl.BlockSpec(memory_space=pltpu.HBM)
    dma = pltpu.SemaphoreType.DMA
    f32, bf16 = jnp.float32, jnp.bfloat16
    shapes = (
        jax.ShapeDtypeStruct((whole, q_cols), bf16),
        jax.ShapeDtypeStruct((kv_cols, whole), bf16),
        jax.ShapeDtypeStruct((kv_cols, whole), bf16),
        jax.ShapeDtypeStruct((1, q_cols), f32),
        jax.ShapeDtypeStruct((1, kv_cols), f32),
        jax.ShapeDtypeStruct((1, kv_cols), f32),
    )
    landed = pl.pallas_call(
        functools.partial(gather_kernel, ranks, d_model),
        out_shape=tuple(pltpu.VMEM(x.shape, x.dtype) for x in shapes),
        in_specs=[hbm] * 8,
        out_specs=(vmem,) * 6,
        scratch_shapes=[
            pltpu.VMEM((2, 1, rows), f32),
            pltpu.VMEM((2, rows, q_cols), f32),
            pltpu.VMEM((2, 2 * kv_cols, rows), f32),
            pltpu.VMEM((rows, 128), f32),
            pltpu.VMEM((rows, 128), f32),
            pltpu.VMEM((ranks, 16, 128), f32),
            dma((2 + SLABS,)),
            dma((2,)),
            dma((1,)),
            dma((2,)),
            dma((2, 2, steps, max(CHUNKS, 2))),
        ],
        compiler_params=pltpu.CompilerParams(
            collective_id=0, has_side_effects=True, vmem_limit_bytes=VMEM_A
        ),
    )(*(
        pltpu.with_memory_space_constraint(x, pltpu.HBM)
        for x in (
            mix_share.reshape(1, rows), norm_gain.reshape(1, rows), one_query, other_query,
            one_key.T, other_key.T, one_value.T, other_value.T,
        )
    ))
    out = pl.pallas_call(
        write_kernel,
        out_shape=shapes,
        in_specs=[vmem] * 6,
        out_specs=(hbm,) * 6,
        scratch_shapes=[dma((8,)), dma((5,))],
        compiler_params=pltpu.CompilerParams(vmem_limit_bytes=VMEM_B),
    )(*landed)
    sq, sk, sv, cq, ck, cv = out
    return sq, sk.T, sv.T, cq[0], ck[0], cv[0]


VMEM_A = 10 * 1024 * 1024
VMEM_B = 2 * 1024 * 1024


def solution(mesh):
    def body(one_query, *rest):
        ranks = mesh.shape["rows"]
        return local(ranks, ranks * one_query.shape[0], one_query, *rest)

    return jax.shard_map(
        body,
        mesh=mesh,
        in_specs=(P("rows", "cols"),) * 6 + (P("rows"),) * 2,
        out_specs=(P(None, "cols"),) * 3 + (P("cols"),) * 3,
        check_vma=False,
    )
```

```python
import functools
import math

import jax
import jax.numpy as jnp
from jax import lax
from jax.experimental import pallas as pl
from jax.experimental.pallas import tpu as pltpu
from jax.sharding import PartitionSpec as P

MESH = pl.DeviceIdType.MESH
EARLY = 48
SLABS = 4
STEP_ROWS = 32


def chip_at(cycle, place, side):
    major = lax.div(place, side)
    minor = lax.rem(place - major + side, side)
    y, x = (minor, major) if cycle == 0 else (major, minor)
    return y * side + x


def place_of(cycle, chip, side):
    y, x = lax.div(chip, side), lax.rem(chip, side)
    major, minor = (x, y) if cycle == 0 else (y, x)
    return major * side + lax.rem(minor + major, side)


def gather_kernel(
    ranks, d_model,
    mix_hbm, gain_hbm, oq, tq, ok, tk, ov, tv,
    sq, sk, sv, cq, ck, cv,
    coefs, q_in, kv_in, col_a, col_b, sums,
    early,
    load_sem, stat_sem, ring_sem, twin_sem, ring_recv, early_sem,
):
    me = lax.axis_index("rows")
    chips = ranks // 2
    side = math.isqrt(chips)
    steps = chips // 2
    chip, core = lax.div(me, 2), lax.rem(me, 2)
    twin = chip * 2 + 1 - core
    rows, q_cols = oq.shape
    kv_cols = ok.shape[0]
    half = rows // 2
    slab = rows // SLABS
    tiles = q_cols // 128
    one, one_kv = q_in.at[0], kv_in.at[0]

    barrier = pltpu.get_barrier_semaphore()
    for shift in range(1, ranks):
        pl.semaphore_signal(
            barrier, inc=1, device_id={"rows": lax.rem(me + shift, ranks)}, device_id_type=MESH
        )

    def load(source, held, sem):
        pltpu.make_async_copy(source, held, sem).start()

    def settle(ref, sem):
        pltpu.make_async_copy(ref, ref, sem).wait()

    load(mix_hbm, coefs.at[0], load_sem.at[0])
    load(gain_hbm, coefs.at[1], load_sem.at[0])
    for s in range(SLABS):
        r = pl.ds(s * slab, slab)
        for n, source in enumerate((oq, tq)):
            load(source.at[r], q_in.at[n, r], load_sem.at[2 + s])
    for n, source in enumerate((ok, tk, ov, tv)):
        load(source, kv_in.at[n % 2, pl.ds(n // 2 * kv_cols, kv_cols)], load_sem.at[1])

    settle(coefs, load_sem.at[0])
    a_row = coefs[1] * coefs[0]
    b_row = coefs[1] * (1.0 - coefs[0])
    for c in range(0, rows, 128):
        col_a[pl.ds(c, 128), :] = jnp.broadcast_to(a_row[:, c:c + 128], (128, 128)).T
        col_b[pl.ds(c, 128), :] = jnp.broadcast_to(b_row[:, c:c + 128], (128, 128)).T

    accs = tuple(jnp.zeros((8, 128), jnp.float32) for _ in range(tiles))
    for s in range(SLABS):
        settle(q_in.at[:, pl.ds(s * slab, slab)], load_sem.at[2 + s])

        def body(i, accs):
            r = pl.ds(pl.multiple_of(s * slab + i * STEP_ROWS, STEP_ROWS), STEP_ROWS)
            a, b = col_a[r, :], col_b[r, :]
            new = []
            for j, acc in enumerate(accs):
                c = pl.ds(j * 128, 128)
                f = a * q_in[0, r, c] + b * q_in[1, r, c]
                one[r, c] = f
                new.append(acc + jnp.sum(jnp.abs(f).reshape(STEP_ROWS // 8, 8, 128), axis=0))
            return tuple(new)

        accs = lax.fori_loop(0, slab // STEP_ROWS, body, accs)
    for j, acc in enumerate(accs):
        sums[me, pl.ds(j, 1), :] = jnp.sum(acc, axis=0, keepdims=True)
    settle(kv_in, load_sem.at[1])
    f = a_row * kv_in[0] + b_row * kv_in[1]
    one_kv[...] = f
    sizes = jnp.abs(f)
    size = sizes[:, 0:128]
    for c in range(128, rows, 128):
        size = size + sizes[:, c:c + 128]
    sums[me, pl.ds(tiles, 1), :] = jnp.sum(size.T, axis=0, keepdims=True)

    def remote(src, dst, send, recv, device):
        pltpu.make_async_remote_copy(
            src_ref=src, dst_ref=dst, send_sem=send, recv_sem=recv,
            device_id={"rows": device}, device_id_type=MESH,
        ).start()

    pl.semaphore_wait(barrier, ranks - 1)
    place = sums.at[me, pl.ds(0, tiles + 1)]
    for shift in range(1, ranks):
        remote(place, place, stat_sem.at[0], stat_sem.at[1], lax.rem(me + shift, ranks))

    spots = [place_of(c, chip, side) for c in range(2)]
    aims = {}
    for c in range(2):
        aims[c, 0] = chip_at(c, lax.rem(spots[c] + 1, chips), side) * 2 + core
        aims[c, 1] = chip_at(c, lax.rem(spots[c] + chips - 1, chips), side) * 2 + core

    def early_rows(way):
        return 0 if way == 0 else half - EARLY

    for c in range(2):
        for way in range(2):
            remote(one.at[pl.ds(c * half + early_rows(way), EARLY)], early.at[c, way],
                   ring_sem.at[1], early_sem.at[c, way], aims[c, way])

    peers = sums.at[pl.ds(0, ranks - 1), pl.ds(0, tiles + 1)]
    settle(peers, stat_sem.at[1])
    total = sums[0, 0:tiles + 1, :]
    for owner in range(1, ranks):
        total = total + sums[owner, 0:tiles + 1, :]
    scale = total / d_model
    inverse = 1.0 / scale

    def pieces(step, way):
        if step < steps:
            cut = half // 2
            cuts = [(0, cut, 2), (cut, half - cut, None)]
            if step == 1:
                cuts[0] = (EARLY, cut - EARLY, 2)
        else:
            cut = half // 4
            cuts = [(0, cut, way), (cut, half // 2 - cut, None)]
        if way == 0:
            return cuts
        return [(half - first - count, count, share) for first, count, share in cuts]

    def refs(c, dev, item):
        first, count, share = item
        at = pl.multiple_of(dev * rows + c * half + first, 16)
        out = [sq.at[pl.ds(at, count)]] if count else []
        if share is not None:
            at = pl.ds(pl.multiple_of(dev * rows, rows), rows)
            ref = (sk, sv)[c]
            if share < 2:
                ref = ref.at[pl.ds(share * (kv_cols // 2), kv_cols // 2)]
            out.append(ref.at[:, at])
        return out

    def ring(c, way, step, at, dev):
        for ref in refs(c, dev, pieces(step, way)[at]):
            remote(ref, ref, ring_sem.at[0], ring_recv.at[c, way, step - 1, at], aims[c, way])

    def settle_ring(c, way, step, at):
        first, count, share = pieces(step, way)[at]
        extra = 0 if share is None else kv_cols * rows // q_cols // (1 if share == 2 else 2)
        settle(sq.at[pl.ds(0, count + extra)], ring_recv.at[c, way, step - 1, at])

    def pass_on(c, dev, item):
        for ref in refs(c, dev, item):
            remote(ref, ref, twin_sem.at[0], twin_sem.at[1], twin)

    def narrow(source, first, dev, to, count):
        def body(i, carry):
            r = pl.ds(pl.multiple_of(first + i * 16, 16), 16)
            out = pl.ds(pl.multiple_of(dev * rows + to + i * 16, 16), 16)
            for j in range(tiles):
                col = pl.ds(j * 128, 128)
                sq[out, col] = (source[r, col] * inverse[j:j + 1, :]).astype(jnp.bfloat16)
            return carry

        lax.fori_loop(0, count // 16, body, 0)

    flip = jnp.broadcast_to(inverse[tiles:tiles + 1, :], (128, 128)).T

    def narrow_kv(c, source, dev):
        at = pl.multiple_of(dev * rows, rows)
        for col in range(0, rows, 128):
            (sk, sv)[c][:, pl.ds(pl.multiple_of(at + col, 128), 128)] = (
                source[:, pl.ds(col, 128)] * flip[c * kv_cols:(c + 1) * kv_cols, :]
            ).astype(jnp.bfloat16)

    def origins(c, step):
        back = chip_at(c, lax.rem(spots[c] + chips - step, chips), side) * 2 + core
        return back, chip_at(c, lax.rem(spots[c] + step, chips), side) * 2 + core

    for c in range(2):
        narrow_kv(c, one_kv.at[pl.ds(c * kv_cols, kv_cols)], me)
        narrow(one, c * half, me, c * half, half)
        for at in range(2):
            for way in range(2):
                ring(c, way, 1, at, me)
    for c in range(2):
        pass_on(c, me, (0, half, 2))

    for j in range(tiles):
        cq[:, pl.ds(j * 128, 128)] = scale[j:j + 1, :]
    ck[...] = scale[tiles:tiles + 1, 0:kv_cols]
    cv[...] = scale[tiles:tiles + 1, kv_cols:2 * kv_cols]

    for step in range(1, steps + 1):
        devs = {c: origins(c, step) for c in range(2)}
        for at in range(2):
            for c in range(2):
                for way in range(2):
                    dev = devs[c][way]
                    if step == 1 and at == 0:
                        settle(q_in.at[0, pl.ds(0, EARLY)], early_sem.at[c, way])
                        narrow(early.at[c, way], 0, dev, c * half + early_rows(way), EARLY)
                    settle_ring(c, way, step, at)
                    item = pieces(step, way)[at]
                    if step == 1:
                        item = pieces(0, way)[at]
                    if step < steps:
                        for later, nxt in enumerate(pieces(step + 1, way)):
                            if item[0] <= nxt[0] < item[0] + item[1]:
                                ring(c, way, step + 1, later, dev)
                    pass_on(c, dev, item)
    settle(peers, stat_sem.at[0])
    share = half + kv_cols * rows // q_cols
    settle(sq.at[pl.ds(0, 2 * (chips - 1) * share - 4 * EARLY)], ring_sem.at[0])
    settle(q_in.at[:, pl.ds(0, 2 * EARLY)], ring_sem.at[1])
    settle(sq.at[pl.ds(0, 2 * chips * share)], twin_sem.at[0])
    settle(sq.at[pl.ds(0, 2 * chips * share)], twin_sem.at[1])


def write_kernel(sq, sk, sv, cq, ck, cv, oq, ok, ov, dq, dk, dv, q_sem, sem):
    count = q_sem.shape[0]
    rows = sq.shape[0] // count
    copies = []
    for n in range(count):
        r = pl.ds(n * rows, rows)
        copies.append(pltpu.make_async_copy(sq.at[r], oq.at[r], q_sem.at[n]))
    for n, (source, out) in enumerate(((sk, ok), (sv, ov), (cq, dq), (ck, dk), (cv, dv))):
        copies.append(pltpu.make_async_copy(source, out, sem.at[n]))
    for copy in copies:
        copy.start()
    for copy in copies:
        copy.wait()


def local(ranks, d_model, one_query, other_query, one_key, other_key, one_value, other_value, mix_share, norm_gain):
    rows, q_cols = one_query.shape
    kv_cols = one_key.shape[1]
    whole = ranks * rows
    steps = ranks // 4
    vmem = pl.BlockSpec(memory_space=pltpu.VMEM)
    hbm = pl.BlockSpec(memory_space=pltpu.HBM)
    dma = pltpu.SemaphoreType.DMA
    f32, bf16 = jnp.float32, jnp.bfloat16
    shapes = (
        jax.ShapeDtypeStruct((whole, q_cols), bf16),
        jax.ShapeDtypeStruct((kv_cols, whole), bf16),
        jax.ShapeDtypeStruct((kv_cols, whole), bf16),
        jax.ShapeDtypeStruct((1, q_cols), f32),
        jax.ShapeDtypeStruct((1, kv_cols), f32),
        jax.ShapeDtypeStruct((1, kv_cols), f32),
    )
    landed = pl.pallas_call(
        functools.partial(gather_kernel, ranks, d_model),
        out_shape=tuple(pltpu.VMEM(x.shape, x.dtype) for x in shapes),
        in_specs=[hbm] * 8,
        out_specs=(vmem,) * 6,
        scratch_shapes=[
            pltpu.VMEM((2, 1, rows), f32),
            pltpu.VMEM((2, rows, q_cols), f32),
            pltpu.VMEM((2, 2 * kv_cols, rows), f32),
            pltpu.VMEM((rows, 128), f32),
            pltpu.VMEM((rows, 128), f32),
            pltpu.VMEM((ranks, 16, 128), f32),
            pltpu.VMEM((2, 2, EARLY, q_cols), f32),
            dma((2 + SLABS,)),
            dma((2,)),
            dma((2,)),
            dma((2,)),
            dma((2, 2, steps, 2)),
            dma((2, 2)),
        ],
        compiler_params=pltpu.CompilerParams(
            collective_id=0, has_side_effects=True, vmem_limit_bytes=VMEM_A
        ),
    )(*(
        pltpu.with_memory_space_constraint(x, pltpu.HBM)
        for x in (
            mix_share.reshape(1, rows), norm_gain.reshape(1, rows), one_query, other_query,
            one_key.T, other_key.T, one_value.T, other_value.T,
        )
    ))
    out = pl.pallas_call(
        write_kernel,
        out_shape=shapes,
        in_specs=[vmem] * 6,
        out_specs=(hbm,) * 6,
        scratch_shapes=[dma((8,)), dma((5,))],
        compiler_params=pltpu.CompilerParams(vmem_limit_bytes=VMEM_B),
    )(*landed)
    sq, sk, sv, cq, ck, cv = out
    return sq, sk.T, sv.T, cq[0], ck[0], cv[0]


VMEM_A = 10 * 1024 * 1024
VMEM_B = 2 * 1024 * 1024


def solution(mesh):
    def body(one_query, *rest):
        ranks = mesh.shape["rows"]
        return local(ranks, ranks * one_query.shape[0], one_query, *rest)

    return jax.shard_map(
        body,
        mesh=mesh,
        in_specs=(P("rows", "cols"),) * 6 + (P("rows"),) * 2,
        out_specs=(P(None, "cols"),) * 3 + (P("cols"),) * 3,
        check_vma=False,
    )
```

```python
import functools
import math

import jax
import jax.numpy as jnp
from jax import lax
from jax.experimental import pallas as pl
from jax.experimental.pallas import tpu as pltpu
from jax.sharding import PartitionSpec as P

MESH = pl.DeviceIdType.MESH
EARLY = 48
SLABS = 2
WRITES = 32
STEP_ROWS = 32


def chip_at(cycle, place, side):
    major = lax.div(place, side)
    minor = lax.rem(place - major + side, side)
    y, x = (minor, major) if cycle == 0 else (major, minor)
    return y * side + x


def place_of(cycle, chip, side):
    y, x = lax.div(chip, side), lax.rem(chip, side)
    major, minor = (x, y) if cycle == 0 else (y, x)
    return major * side + lax.rem(minor + major, side)


def gather_kernel(
    ranks, d_model,
    mix_hbm, gain_hbm, oq, tq, ok, tk, ov, tv,
    sq, sk, sv, cq, ck, cv,
    coefs, q_in, kv_in, col_a, col_b, sums,
    early,
    load_sem, stat_sem, ring_sem, twin_sem, ring_recv, early_sem,
):
    me = lax.axis_index("rows")
    chips = ranks // 2
    side = math.isqrt(chips)
    steps = chips // 2
    chip, core = lax.div(me, 2), lax.rem(me, 2)
    twin = chip * 2 + 1 - core
    rows, q_cols = oq.shape
    kv_cols = ok.shape[0]
    half = rows // 2
    slab = rows // SLABS
    tiles = q_cols // 128
    one, one_kv = q_in.at[0], kv_in.at[0]

    y, x = lax.div(chip, side), lax.rem(chip, side)
    hops = [min(k, side - k) for k in range(side)]
    away = sorted(
        ((dy, dx) for dy in range(side) for dx in range(side) if dy or dx),
        key=lambda d: -(hops[d[0]] + hops[d[1]]),
    )
    others = [
        (lax.rem(y + dy, side) * side + lax.rem(x + dx, side)) * 2 + k
        for dy, dx in away for k in range(2)
    ] + [twin]

    barrier = pltpu.get_barrier_semaphore()
    for dev in others:
        pl.semaphore_signal(barrier, inc=1, device_id={"rows": dev}, device_id_type=MESH)

    def load(source, held, sem):
        pltpu.make_async_copy(source, held, sem).start()

    def settle(ref, sem):
        pltpu.make_async_copy(ref, ref, sem).wait()

    load(mix_hbm, coefs.at[0], load_sem.at[0])
    load(gain_hbm, coefs.at[1], load_sem.at[0])
    for s in range(SLABS):
        r = pl.ds(s * slab, slab)
        for n, source in enumerate((oq, tq)):
            load(source.at[r], q_in.at[n, r], load_sem.at[2 + s])
    for n, source in enumerate((ok, tk, ov, tv)):
        load(source, kv_in.at[n % 2, pl.ds(n // 2 * kv_cols, kv_cols)], load_sem.at[1])

    settle(coefs, load_sem.at[0])
    a_row = coefs[1] * coefs[0]
    b_row = coefs[1] * (1.0 - coefs[0])
    for c in range(0, rows, 128):
        col_a[pl.ds(c, 128), :] = jnp.broadcast_to(a_row[:, c:c + 128], (128, 128)).T
        col_b[pl.ds(c, 128), :] = jnp.broadcast_to(b_row[:, c:c + 128], (128, 128)).T

    accs = tuple(jnp.zeros((8, 128), jnp.float32) for _ in range(tiles))
    for s in range(SLABS):
        settle(q_in.at[:, pl.ds(s * slab, slab)], load_sem.at[2 + s])

        def body(i, accs):
            r = pl.ds(pl.multiple_of(s * slab + i * STEP_ROWS, STEP_ROWS), STEP_ROWS)
            a, b = col_a[r, :], col_b[r, :]
            new = []
            for j, acc in enumerate(accs):
                c = pl.ds(j * 128, 128)
                f = a * q_in[0, r, c] + b * q_in[1, r, c]
                one[r, c] = f
                new.append(acc + jnp.sum(jnp.abs(f).reshape(STEP_ROWS // 8, 8, 128), axis=0))
            return tuple(new)

        accs = lax.fori_loop(0, slab // STEP_ROWS, body, accs)
    for j, acc in enumerate(accs):
        sums[me, pl.ds(j, 1), :] = jnp.sum(acc, axis=0, keepdims=True)
    settle(kv_in, load_sem.at[1])
    f = a_row * kv_in[0] + b_row * kv_in[1]
    one_kv[...] = f
    sizes = jnp.abs(f)
    size = sizes[:, 0:128]
    for c in range(128, rows, 128):
        size = size + sizes[:, c:c + 128]
    sums[me, pl.ds(tiles, 1), :] = jnp.sum(size.T, axis=0, keepdims=True)

    def remote(src, dst, send, recv, device):
        pltpu.make_async_remote_copy(
            src_ref=src, dst_ref=dst, send_sem=send, recv_sem=recv,
            device_id={"rows": device}, device_id_type=MESH,
        ).start()

    pl.semaphore_wait(barrier, ranks - 1)
    place = sums.at[me, pl.ds(0, tiles + 1)]
    for dev in others:
        remote(place, place, stat_sem.at[0], stat_sem.at[1], dev)

    spots = [place_of(c, chip, side) for c in range(2)]
    aims = {}
    for c in range(2):
        aims[c, 0] = chip_at(c, lax.rem(spots[c] + 1, chips), side) * 2 + core
        aims[c, 1] = chip_at(c, lax.rem(spots[c] + chips - 1, chips), side) * 2 + core

    def early_rows(way):
        return 0 if way == 0 else half - EARLY

    for c in range(2):
        for way in range(2):
            remote(one.at[pl.ds(c * half + early_rows(way), EARLY)], early.at[c, way],
                   ring_sem.at[1], early_sem.at[c, way], aims[c, way])

    peers = sums.at[pl.ds(0, ranks - 1), pl.ds(0, tiles + 1)]
    settle(peers, stat_sem.at[1])
    total = sums[0, 0:tiles + 1, :]
    for owner in range(1, ranks):
        total = total + sums[owner, 0:tiles + 1, :]
    scale = total / d_model
    inverse = 1.0 / scale

    def pieces(step, way):
        if step < steps:
            cut = half // 2
            cuts = [(0, cut, 2), (cut, half - cut, None)]
            if step == 1:
                cuts[0] = (EARLY, cut - EARLY, 2)
        else:
            cut = half // 4
            cuts = [(0, cut, way), (cut, half // 2 - cut, None)]
        if way == 0:
            return cuts
        return [(half - first - count, count, share) for first, count, share in cuts]

    def refs(c, dev, item):
        first, count, share = item
        at = pl.multiple_of(dev * rows + c * half + first, 16)
        out = [sq.at[pl.ds(at, count)]] if count else []
        if share is not None:
            at = pl.ds(pl.multiple_of(dev * rows, rows), rows)
            ref = (sk, sv)[c]
            if share < 2:
                ref = ref.at[pl.ds(share * (kv_cols // 2), kv_cols // 2)]
            out.append(ref.at[:, at])
        return out

    def ring(c, way, step, at, dev):
        for ref in refs(c, dev, pieces(step, way)[at]):
            remote(ref, ref, ring_sem.at[0], ring_recv.at[way, step - 1, at], aims[c, way])

    def settle_ring(way, step, at):
        first, count, share = pieces(step, way)[at]
        extra = 0 if share is None else kv_cols * rows // q_cols // (1 if share == 2 else 2)
        settle(sq.at[pl.ds(0, 2 * (count + extra))], ring_recv.at[way, step - 1, at])

    def pass_on(c, dev, item):
        for ref in refs(c, dev, item):
            remote(ref, ref, twin_sem.at[0], twin_sem.at[1], twin)

    def narrow(source, first, dev, to, count):
        def body(i, carry):
            r = pl.ds(pl.multiple_of(first + i * 16, 16), 16)
            out = pl.ds(pl.multiple_of(dev * rows + to + i * 16, 16), 16)
            for j in range(tiles):
                col = pl.ds(j * 128, 128)
                sq[out, col] = (source[r, col] * inverse[j:j + 1, :]).astype(jnp.bfloat16)
            return carry

        lax.fori_loop(0, count // 16, body, 0)

    flip = jnp.broadcast_to(inverse[tiles:tiles + 1, :], (128, 128)).T

    def narrow_kv(c, source, dev):
        at = pl.multiple_of(dev * rows, rows)
        for col in range(0, rows, 128):
            (sk, sv)[c][:, pl.ds(pl.multiple_of(at + col, 128), 128)] = (
                source[:, pl.ds(col, 128)] * flip[c * kv_cols:(c + 1) * kv_cols, :]
            ).astype(jnp.bfloat16)

    def origins(c, step):
        back = chip_at(c, lax.rem(spots[c] + chips - step, chips), side) * 2 + core
        return back, chip_at(c, lax.rem(spots[c] + step, chips), side) * 2 + core

    for c in range(2):
        narrow_kv(c, one_kv.at[pl.ds(c * kv_cols, kv_cols)], me)
        narrow(one, c * half, me, c * half, half)
        for at in range(2):
            for way in range(2):
                ring(c, way, 1, at, me)
    for c in range(2):
        pass_on(c, me, (0, half, 2))

    for j in range(tiles):
        cq[:, pl.ds(j * 128, 128)] = scale[j:j + 1, :]
    ck[...] = scale[tiles:tiles + 1, 0:kv_cols]
    cv[...] = scale[tiles:tiles + 1, kv_cols:2 * kv_cols]

    for step in range(1, steps + 1):
        devs = {c: origins(c, step) for c in range(2)}
        for at in range(2):
            for way in range(2):
                if step == 1 and at == 0:
                    for c in range(2):
                        settle(q_in.at[0, pl.ds(0, EARLY)], early_sem.at[c, way])
                        narrow(early.at[c, way], 0, devs[c][way], c * half + early_rows(way), EARLY)
                settle_ring(way, step, at)
                item = pieces(min(step, steps) if step > 1 else 0, way)[at]
                for c in range(2):
                    if step < steps:
                        for later, nxt in enumerate(pieces(step + 1, way)):
                            if item[0] <= nxt[0] < item[0] + item[1]:
                                ring(c, way, step + 1, later, devs[c][way])
                for c in range(2):
                    pass_on(c, devs[c][way], item)
    settle(peers, stat_sem.at[0])
    share = half + kv_cols * rows // q_cols
    settle(sq.at[pl.ds(0, 2 * (chips - 1) * share - 4 * EARLY)], ring_sem.at[0])
    settle(q_in.at[:, pl.ds(0, 2 * EARLY)], ring_sem.at[1])
    settle(sq.at[pl.ds(0, 2 * chips * share)], twin_sem.at[0])
    settle(sq.at[pl.ds(0, 2 * chips * share)], twin_sem.at[1])


def write_kernel(sq, sk, sv, cq, ck, cv, oq, ok, ov, dq, dk, dv, sem):
    rows = sq.shape[0] // WRITES
    pairs = [(cq, dq), (ck, dk), (cv, dv), (sk, ok), (sv, ov)]
    for n in range(WRITES):
        r = pl.ds(n * rows, rows)
        pairs.append((sq.at[r], oq.at[r]))
    for n, (source, out) in enumerate(pairs):
        pltpu.make_async_copy(source, out, sem.at[min(n, 5)]).start()
    for n, (source, out) in enumerate(pairs[:5] + [(sq, oq)]):
        pltpu.make_async_copy(source, out, sem.at[n]).wait()


def local(ranks, d_model, one_query, other_query, one_key, other_key, one_value, other_value, mix_share, norm_gain):
    rows, q_cols = one_query.shape
    kv_cols = one_key.shape[1]
    whole = ranks * rows
    steps = ranks // 4
    vmem = pl.BlockSpec(memory_space=pltpu.VMEM)
    hbm = pl.BlockSpec(memory_space=pltpu.HBM)
    dma = pltpu.SemaphoreType.DMA
    f32, bf16 = jnp.float32, jnp.bfloat16
    shapes = (
        jax.ShapeDtypeStruct((whole, q_cols), bf16),
        jax.ShapeDtypeStruct((kv_cols, whole), bf16),
        jax.ShapeDtypeStruct((kv_cols, whole), bf16),
        jax.ShapeDtypeStruct((1, q_cols), f32),
        jax.ShapeDtypeStruct((1, kv_cols), f32),
        jax.ShapeDtypeStruct((1, kv_cols), f32),
    )
    landed = pl.pallas_call(
        functools.partial(gather_kernel, ranks, d_model),
        out_shape=tuple(pltpu.VMEM(x.shape, x.dtype) for x in shapes),
        in_specs=[hbm] * 8,
        out_specs=(vmem,) * 6,
        scratch_shapes=[
            pltpu.VMEM((2, 1, rows), f32),
            pltpu.VMEM((2, rows, q_cols), f32),
            pltpu.VMEM((2, 2 * kv_cols, rows), f32),
            pltpu.VMEM((rows, 128), f32),
            pltpu.VMEM((rows, 128), f32),
            pltpu.VMEM((ranks, 16, 128), f32),
            pltpu.VMEM((2, 2, EARLY, q_cols), f32),
            dma((2 + SLABS,)),
            dma((2,)),
            dma((2,)),
            dma((2,)),
            dma((2, steps, 2)),
            dma((2, 2)),
        ],
        compiler_params=pltpu.CompilerParams(
            collective_id=0, has_side_effects=True, vmem_limit_bytes=VMEM_A
        ),
    )(*(
        pltpu.with_memory_space_constraint(x, pltpu.HBM)
        for x in (
            mix_share.reshape(1, rows), norm_gain.reshape(1, rows), one_query, other_query,
            one_key.T, other_key.T, one_value.T, other_value.T,
        )
    ))
    out = pl.pallas_call(
        write_kernel,
        out_shape=shapes,
        in_specs=[vmem] * 6,
        out_specs=(hbm,) * 6,
        scratch_shapes=[dma((6,))],
        compiler_params=pltpu.CompilerParams(vmem_limit_bytes=VMEM_B),
    )(*landed)
    sq, sk, sv, cq, ck, cv = out
    return sq, sk.T, sv.T, cq[0], ck[0], cv[0]


VMEM_A = 10 * 1024 * 1024
VMEM_B = 2 * 1024 * 1024


def solution(mesh):
    def body(one_query, *rest):
        ranks = mesh.shape["rows"]
        return local(ranks, ranks * one_query.shape[0], one_query, *rest)

    return jax.shard_map(
        body,
        mesh=mesh,
        in_specs=(P("rows", "cols"),) * 6 + (P("rows"),) * 2,
        out_specs=(P(None, "cols"),) * 3 + (P("cols"),) * 3,
        check_vma=False,
    )
```

```python
import functools
import math

import jax
import jax.numpy as jnp
from jax import lax
from jax.experimental import pallas as pl
from jax.experimental.pallas import tpu as pltpu
from jax.sharding import PartitionSpec as P

MESH = pl.DeviceIdType.MESH
EARLY = (48, 16)
SLABS = 2
WRITES = 32
STEP_ROWS = 32


def chip_at(cycle, place, side):
    major = lax.div(place, side)
    minor = lax.rem(place - major + side, side)
    y, x = (minor, major) if cycle == 0 else (major, minor)
    return y * side + x


def place_of(cycle, chip, side):
    y, x = lax.div(chip, side), lax.rem(chip, side)
    major, minor = (x, y) if cycle == 0 else (y, x)
    return major * side + lax.rem(minor + major, side)


def gather_kernel(
    ranks, d_model,
    mix_hbm, gain_hbm, oq, tq, ok, tk, ov, tv,
    sq, sk, sv, cq, ck, cv,
    coefs, q_in, kv_in, col_a, col_b, line, column, early,
    load_sem, stat_sem, ring_sem, twin_sem, ring_recv, early_sem,
):
    me = lax.axis_index("rows")
    chips = ranks // 2
    side = math.isqrt(chips)
    steps = chips // 2
    chip, core = lax.div(me, 2), lax.rem(me, 2)
    twin = chip * 2 + 1 - core
    rows, q_cols = oq.shape
    kv_cols = ok.shape[0]
    half = rows // 2
    slab = rows // SLABS
    tiles = q_cols // 128
    one, one_kv = q_in.at[0], kv_in.at[0]

    y, x = lax.div(chip, side), lax.rem(chip, side)
    order = sorted(range(1, side), key=lambda k: -min(k, side - k))
    row_peers = [
        (y * side + lax.rem(x + k, side)) * 2 + n for k in order for n in range(2)
    ] + [twin]
    column_peers = [(lax.rem(y + k, side) * side + x) * 2 + core for k in order]

    barrier = pltpu.get_barrier_semaphore()
    for dev in row_peers + column_peers:
        pl.semaphore_signal(barrier, inc=1, device_id={"rows": dev}, device_id_type=MESH)

    def load(source, held, sem):
        pltpu.make_async_copy(source, held, sem).start()

    def settle(ref, sem):
        pltpu.make_async_copy(ref, ref, sem).wait()

    load(mix_hbm, coefs.at[0], load_sem.at[0])
    load(gain_hbm, coefs.at[1], load_sem.at[0])
    for s in range(SLABS):
        r = pl.ds(s * slab, slab)
        for n, source in enumerate((oq, tq)):
            load(source.at[r], q_in.at[n, r], load_sem.at[2 + s])
    for n, source in enumerate((ok, tk, ov, tv)):
        load(source, kv_in.at[n % 2, pl.ds(n // 2 * kv_cols, kv_cols)], load_sem.at[1])

    settle(coefs, load_sem.at[0])
    a_row = coefs[1] * coefs[0]
    b_row = coefs[1] * (1.0 - coefs[0])
    for c in range(0, rows, 128):
        col_a[pl.ds(c, 128), :] = jnp.broadcast_to(a_row[:, c:c + 128], (128, 128)).T
        col_b[pl.ds(c, 128), :] = jnp.broadcast_to(b_row[:, c:c + 128], (128, 128)).T

    spot = x * 2 + core
    accs = tuple(jnp.zeros((8, 128), jnp.float32) for _ in range(tiles))
    for s in range(SLABS):
        settle(q_in.at[:, pl.ds(s * slab, slab)], load_sem.at[2 + s])

        def body(i, accs):
            r = pl.ds(pl.multiple_of(s * slab + i * STEP_ROWS, STEP_ROWS), STEP_ROWS)
            a, b = col_a[r, :], col_b[r, :]
            new = []
            for j, acc in enumerate(accs):
                c = pl.ds(j * 128, 128)
                f = a * q_in[0, r, c] + b * q_in[1, r, c]
                one[r, c] = f
                new.append(acc + jnp.sum(jnp.abs(f).reshape(STEP_ROWS // 8, 8, 128), axis=0))
            return tuple(new)

        accs = lax.fori_loop(0, slab // STEP_ROWS, body, accs)
    for j, acc in enumerate(accs):
        line[spot, pl.ds(j, 1), :] = jnp.sum(acc, axis=0, keepdims=True)
    settle(kv_in, load_sem.at[1])
    f = a_row * kv_in[0] + b_row * kv_in[1]
    one_kv[...] = f
    sizes = jnp.abs(f)
    size = sizes[:, 0:128]
    for c in range(128, rows, 128):
        size = size + sizes[:, c:c + 128]
    line[spot, pl.ds(tiles, 1), :] = jnp.sum(size.T, axis=0, keepdims=True)

    def remote(src, dst, send, recv, device):
        pltpu.make_async_remote_copy(
            src_ref=src, dst_ref=dst, send_sem=send, recv_sem=recv,
            device_id={"rows": device}, device_id_type=MESH,
        ).start()

    pl.semaphore_wait(barrier, len(row_peers) + len(column_peers))
    lines = pl.ds(0, tiles + 1)
    place = line.at[spot, lines]
    for dev in row_peers:
        remote(place, place, stat_sem.at[0], stat_sem.at[1], dev)

    spots = [place_of(c, chip, side) for c in range(2)]
    aims = {}
    for c in range(2):
        aims[c, 0] = chip_at(c, lax.rem(spots[c] + 1, chips), side) * 2 + core
        aims[c, 1] = chip_at(c, lax.rem(spots[c] + chips - 1, chips), side) * 2 + core

    ahead = sum(EARLY)

    def early_rows(way):
        return 0 if way == 0 else half - ahead

    def send_early(batch):
        skip = sum(EARLY[:batch])
        count = EARLY[batch]
        for c in range(2):
            for way in range(2):
                at = skip if way == 0 else ahead - skip - count
                remote(one.at[pl.ds(c * half + early_rows(way) + at, count)],
                       early.at[c, way, pl.ds(at, count)],
                       ring_sem.at[1], early_sem.at[batch, way], aims[c, way])

    def gathered(ref, peers, sems):
        slots = ref.at[pl.ds(0, peers), lines]
        settle(slots, sems)
        total = ref[0, 0:tiles + 1, :]
        for n in range(1, peers + 1):
            total = total + ref[n, 0:tiles + 1, :]
        return total

    send_early(0)
    column[y, lines, :] = gathered(line, len(row_peers), stat_sem.at[1])
    place = column.at[y, lines]
    for dev in column_peers:
        remote(place, place, stat_sem.at[2], stat_sem.at[3], dev)
    send_early(1)
    total = gathered(column, len(column_peers), stat_sem.at[3])
    scale = total / d_model
    inverse = 1.0 / scale

    def pieces(step, way):
        if step < steps:
            cut = half // 2
            cuts = [(0, cut, 2), (cut, half - cut, None)]
            if step == 1:
                cuts[0] = (ahead, cut - ahead, 2)
        else:
            cut = half // 4
            cuts = [(0, cut, way), (cut, half // 2 - cut, None)]
        if way == 0:
            return cuts
        return [(half - first - count, count, share) for first, count, share in cuts]

    def refs(c, dev, item):
        first, count, share = item
        at = pl.multiple_of(dev * rows + c * half + first, 16)
        out = [sq.at[pl.ds(at, count)]] if count else []
        if share is not None:
            at = pl.ds(pl.multiple_of(dev * rows, rows), rows)
            ref = (sk, sv)[c]
            if share < 2:
                ref = ref.at[pl.ds(share * (kv_cols // 2), kv_cols // 2)]
            out.append(ref.at[:, at])
        return out

    def ring(c, way, step, at, dev):
        for ref in refs(c, dev, pieces(step, way)[at]):
            remote(ref, ref, ring_sem.at[0], ring_recv.at[way, step - 1, at], aims[c, way])

    def settle_ring(way, step, at):
        first, count, share = pieces(step, way)[at]
        extra = 0 if share is None else kv_cols * rows // q_cols // (1 if share == 2 else 2)
        settle(sq.at[pl.ds(0, 2 * (count + extra))], ring_recv.at[way, step - 1, at])

    def pass_on(c, dev, item):
        for ref in refs(c, dev, item):
            remote(ref, ref, twin_sem.at[0], twin_sem.at[1], twin)

    def narrow(source, first, dev, to, count):
        def body(i, carry):
            r = pl.ds(pl.multiple_of(first + i * 16, 16), 16)
            out = pl.ds(pl.multiple_of(dev * rows + to + i * 16, 16), 16)
            for j in range(tiles):
                col = pl.ds(j * 128, 128)
                sq[out, col] = (source[r, col] * inverse[j:j + 1, :]).astype(jnp.bfloat16)
            return carry

        lax.fori_loop(0, count // 16, body, 0)

    flip = jnp.broadcast_to(inverse[tiles:tiles + 1, :], (128, 128)).T

    def narrow_kv(c, source, dev):
        at = pl.multiple_of(dev * rows, rows)
        for col in range(0, rows, 128):
            (sk, sv)[c][:, pl.ds(pl.multiple_of(at + col, 128), 128)] = (
                source[:, pl.ds(col, 128)] * flip[c * kv_cols:(c + 1) * kv_cols, :]
            ).astype(jnp.bfloat16)

    def origins(c, step):
        back = chip_at(c, lax.rem(spots[c] + chips - step, chips), side) * 2 + core
        return back, chip_at(c, lax.rem(spots[c] + step, chips), side) * 2 + core

    for c in range(2):
        narrow_kv(c, one_kv.at[pl.ds(c * kv_cols, kv_cols)], me)
        narrow(one, c * half, me, c * half, half)
        for at in range(2):
            for way in range(2):
                ring(c, way, 1, at, me)
    for c in range(2):
        pass_on(c, me, (0, half, 2))

    for j in range(tiles):
        cq[:, pl.ds(j * 128, 128)] = scale[j:j + 1, :]
    ck[...] = scale[tiles:tiles + 1, 0:kv_cols]
    cv[...] = scale[tiles:tiles + 1, kv_cols:2 * kv_cols]

    for step in range(1, steps + 1):
        devs = {c: origins(c, step) for c in range(2)}
        for at in range(2):
            for way in range(2):
                if step == 1 and at == 0:
                    for batch, count in enumerate(EARLY):
                        settle(q_in.at[:, pl.ds(0, count)], early_sem.at[batch, way])
                    for c in range(2):
                        narrow(early.at[c, way], 0, devs[c][way], c * half + early_rows(way), ahead)
                settle_ring(way, step, at)
                item = pieces(min(step, steps) if step > 1 else 0, way)[at]
                for c in range(2):
                    if step < steps:
                        for later, nxt in enumerate(pieces(step + 1, way)):
                            if item[0] <= nxt[0] < item[0] + item[1]:
                                ring(c, way, step + 1, later, devs[c][way])
                for c in range(2):
                    pass_on(c, devs[c][way], item)
    settle(line.at[pl.ds(0, len(row_peers)), lines], stat_sem.at[0])
    settle(column.at[pl.ds(0, len(column_peers)), lines], stat_sem.at[2])
    share = half + kv_cols * rows // q_cols
    settle(sq.at[pl.ds(0, 2 * (chips - 1) * share - 4 * ahead)], ring_sem.at[0])
    settle(q_in.at[:, pl.ds(0, 2 * ahead)], ring_sem.at[1])
    settle(sq.at[pl.ds(0, 2 * chips * share)], twin_sem.at[0])
    settle(sq.at[pl.ds(0, 2 * chips * share)], twin_sem.at[1])


def write_kernel(sq, sk, sv, cq, ck, cv, oq, ok, ov, dq, dk, dv, sem):
    rows = sq.shape[0] // WRITES
    pairs = [(cq, dq), (ck, dk), (cv, dv), (sk, ok), (sv, ov)]
    for n in range(WRITES):
        r = pl.ds(n * rows, rows)
        pairs.append((sq.at[r], oq.at[r]))
    for n, (source, out) in enumerate(pairs):
        pltpu.make_async_copy(source, out, sem.at[min(n, 5)]).start()
    for n, (source, out) in enumerate(pairs[:5] + [(sq, oq)]):
        pltpu.make_async_copy(source, out, sem.at[n]).wait()


def local(ranks, d_model, one_query, other_query, one_key, other_key, one_value, other_value, mix_share, norm_gain):
    rows, q_cols = one_query.shape
    kv_cols = one_key.shape[1]
    whole = ranks * rows
    steps = ranks // 4
    side = math.isqrt(ranks // 2)
    vmem = pl.BlockSpec(memory_space=pltpu.VMEM)
    hbm = pl.BlockSpec(memory_space=pltpu.HBM)
    dma = pltpu.SemaphoreType.DMA
    f32, bf16 = jnp.float32, jnp.bfloat16
    shapes = (
        jax.ShapeDtypeStruct((whole, q_cols), bf16),
        jax.ShapeDtypeStruct((kv_cols, whole), bf16),
        jax.ShapeDtypeStruct((kv_cols, whole), bf16),
        jax.ShapeDtypeStruct((1, q_cols), f32),
        jax.ShapeDtypeStruct((1, kv_cols), f32),
        jax.ShapeDtypeStruct((1, kv_cols), f32),
    )
    landed = pl.pallas_call(
        functools.partial(gather_kernel, ranks, d_model),
        out_shape=tuple(pltpu.VMEM(x.shape, x.dtype) for x in shapes),
        in_specs=[hbm] * 8,
        out_specs=(vmem,) * 6,
        scratch_shapes=[
            pltpu.VMEM((2, 1, rows), f32),
            pltpu.VMEM((2, rows, q_cols), f32),
            pltpu.VMEM((2, 2 * kv_cols, rows), f32),
            pltpu.VMEM((rows, 128), f32),
            pltpu.VMEM((rows, 128), f32),
            pltpu.VMEM((2 * side, 16, 128), f32),
            pltpu.VMEM((side, 16, 128), f32),
            pltpu.VMEM((2, 2, sum(EARLY), q_cols), f32),
            dma((2 + SLABS,)),
            dma((4,)),
            dma((2,)),
            dma((2,)),
            dma((2, steps, 2)),
            dma((2, 2)),
        ],
        compiler_params=pltpu.CompilerParams(
            collective_id=0, has_side_effects=True, vmem_limit_bytes=VMEM_A
        ),
    )(*(
        pltpu.with_memory_space_constraint(x, pltpu.HBM)
        for x in (
            mix_share.reshape(1, rows), norm_gain.reshape(1, rows), one_query, other_query,
            one_key.T, other_key.T, one_value.T, other_value.T,
        )
    ))
    out = pl.pallas_call(
        write_kernel,
        out_shape=shapes,
        in_specs=[vmem] * 6,
        out_specs=(hbm,) * 6,
        scratch_shapes=[dma((6,))],
        compiler_params=pltpu.CompilerParams(vmem_limit_bytes=VMEM_B),
    )(*landed)
    sq, sk, sv, cq, ck, cv = out
    return sq, sk.T, sv.T, cq[0], ck[0], cv[0]


VMEM_A = 10 * 1024 * 1024
VMEM_B = 2 * 1024 * 1024


def solution(mesh):
    def body(one_query, *rest):
        ranks = mesh.shape["rows"]
        return local(ranks, ranks * one_query.shape[0], one_query, *rest)

    return jax.shard_map(
        body,
        mesh=mesh,
        in_specs=(P("rows", "cols"),) * 6 + (P("rows"),) * 2,
        out_specs=(P(None, "cols"),) * 3 + (P("cols"),) * 3,
        check_vma=False,
    )
```

```python
import functools
import math

import jax
import jax.numpy as jnp
from jax import lax
from jax.experimental import pallas as pl
from jax.experimental.pallas import tpu as pltpu
from jax.sharding import PartitionSpec as P

MESH = pl.DeviceIdType.MESH
EARLY = (32, 32)
SLABS = 4
PIECES = 4
WRITES = 32
STEP_ROWS = 32


def chip_at(cycle, place, side):
    major = lax.div(place, side)
    minor = lax.rem(place - major + side, side)
    y, x = (minor, major) if cycle == 0 else (major, minor)
    return y * side + x


def place_of(cycle, chip, side):
    y, x = lax.div(chip, side), lax.rem(chip, side)
    major, minor = (x, y) if cycle == 0 else (y, x)
    return major * side + lax.rem(minor + major, side)


def gather_kernel(
    ranks, d_model,
    mix_hbm, gain_hbm, oq, tq, ok, tk, ov, tv,
    sq, sk, sv, cq, ck, cv,
    coefs, q_in, kv_in, col_a, col_b, line, column, early,
    load_sem, stat_sem, ring_sem, twin_sem, ring_recv, early_sem,
):
    me = lax.axis_index("rows")
    chips = ranks // 2
    side = math.isqrt(chips)
    steps = chips // 2
    chip, core = lax.div(me, 2), lax.rem(me, 2)
    twin = chip * 2 + 1 - core
    rows, q_cols = oq.shape
    kv_cols = ok.shape[0]
    half = rows // 2
    slab = rows // SLABS
    tiles = q_cols // 128
    one, one_kv = q_in.at[0], kv_in.at[0]

    y, x = lax.div(chip, side), lax.rem(chip, side)
    order = sorted(range(1, side), key=lambda k: -min(k, side - k))
    row_peers = [
        (y * side + lax.rem(x + k, side)) * 2 + n for k in order for n in range(2)
    ] + [twin]
    column_peers = [(lax.rem(y + k, side) * side + x) * 2 + core for k in order]

    barrier = pltpu.get_barrier_semaphore()
    for dev in row_peers + column_peers:
        pl.semaphore_signal(barrier, inc=1, device_id={"rows": dev}, device_id_type=MESH)

    def load(source, held, sem):
        pltpu.make_async_copy(source, held, sem).start()

    def settle(ref, sem):
        pltpu.make_async_copy(ref, ref, sem).wait()

    load(mix_hbm, coefs.at[0], load_sem.at[0])
    load(gain_hbm, coefs.at[1], load_sem.at[0])
    for n, source in enumerate((ok, tk, ov, tv)):
        load(source, kv_in.at[n % 2, pl.ds(n // 2 * kv_cols, kv_cols)], load_sem.at[1])
    for s in range(SLABS):
        r = pl.ds(s * slab, slab)
        for n, source in enumerate((oq, tq)):
            load(source.at[r], q_in.at[n, r], load_sem.at[2 + s])

    settle(coefs, load_sem.at[0])
    a_row = coefs[1] * coefs[0]
    b_row = coefs[1] * (1.0 - coefs[0])
    for c in range(0, rows, 128):
        col_a[pl.ds(c, 128), :] = jnp.broadcast_to(a_row[:, c:c + 128], (128, 128)).T
        col_b[pl.ds(c, 128), :] = jnp.broadcast_to(b_row[:, c:c + 128], (128, 128)).T

    spot = x * 2 + core
    settle(kv_in, load_sem.at[1])
    f = a_row * kv_in[0] + b_row * kv_in[1]
    one_kv[...] = f
    sizes = jnp.abs(f)
    size = sizes[:, 0:128]
    for c in range(128, rows, 128):
        size = size + sizes[:, c:c + 128]
    line[spot, pl.ds(tiles, 1), :] = jnp.sum(size.T, axis=0, keepdims=True)

    accs = tuple(jnp.zeros((8, 128), jnp.float32) for _ in range(tiles))
    for s in range(SLABS):
        settle(q_in.at[:, pl.ds(s * slab, slab)], load_sem.at[2 + s])

        def body(i, accs):
            r = pl.ds(pl.multiple_of(s * slab + i * STEP_ROWS, STEP_ROWS), STEP_ROWS)
            a, b = col_a[r, :], col_b[r, :]
            new = []
            for j, acc in enumerate(accs):
                c = pl.ds(j * 128, 128)
                f = a * q_in[0, r, c] + b * q_in[1, r, c]
                one[r, c] = f
                new.append(acc + jnp.sum(jnp.abs(f).reshape(STEP_ROWS // 8, 8, 128), axis=0))
            return tuple(new)

        accs = lax.fori_loop(0, slab // STEP_ROWS, body, accs)
    for j, acc in enumerate(accs):
        line[spot, pl.ds(j, 1), :] = jnp.sum(acc, axis=0, keepdims=True)

    def remote(src, dst, send, recv, device):
        pltpu.make_async_remote_copy(
            src_ref=src, dst_ref=dst, send_sem=send, recv_sem=recv,
            device_id={"rows": device}, device_id_type=MESH,
        ).start()

    pl.semaphore_wait(barrier, len(row_peers) + len(column_peers))
    lines = pl.ds(0, tiles + 1)
    place = line.at[spot, lines]
    for dev in row_peers:
        remote(place, place, stat_sem.at[0], stat_sem.at[1], dev)

    spots = [place_of(c, chip, side) for c in range(2)]
    aims = {}
    for c in range(2):
        aims[c, 0] = chip_at(c, lax.rem(spots[c] + 1, chips), side) * 2 + core
        aims[c, 1] = chip_at(c, lax.rem(spots[c] + chips - 1, chips), side) * 2 + core

    ahead = sum(EARLY)

    def early_rows(way):
        return 0 if way == 0 else half - ahead

    def send_early(batch):
        skip = sum(EARLY[:batch])
        count = EARLY[batch]
        for c in range(2):
            for way in range(2):
                at = skip if way == 0 else ahead - skip - count
                remote(one.at[pl.ds(c * half + early_rows(way) + at, count)],
                       early.at[c, way, pl.ds(at, count)],
                       ring_sem.at[1], early_sem.at[batch, way], aims[c, way])

    def gathered(ref, peers, sems):
        slots = ref.at[pl.ds(0, peers), lines]
        settle(slots, sems)
        total = ref[0, 0:tiles + 1, :]
        for n in range(1, peers + 1):
            total = total + ref[n, 0:tiles + 1, :]
        return total

    send_early(0)
    column[y, lines, :] = gathered(line, len(row_peers), stat_sem.at[1])
    place = column.at[y, lines]
    for dev in column_peers:
        remote(place, place, stat_sem.at[2], stat_sem.at[3], dev)
    send_early(1)
    total = gathered(column, len(column_peers), stat_sem.at[3])
    scale = total / d_model
    inverse = 1.0 / scale

    def pieces(step, way):
        part = half // PIECES
        cuts = []
        for at in range(PIECES if step < steps else PIECES // 2):
            first, last = at * part, (at + 1) * part
            if step == 1:
                first = min(max(first, ahead), last)
            share = None if at else (2 if step < steps else way)
            cuts.append((first, last - first, share))
        if way == 0:
            return cuts
        return [(half - first - count, count, share) for first, count, share in cuts]

    def refs(c, dev, item):
        first, count, share = item
        at = pl.multiple_of(dev * rows + c * half + first, 16)
        out = [sq.at[pl.ds(at, count)]] if count else []
        if share is not None:
            at = pl.ds(pl.multiple_of(dev * rows, rows), rows)
            ref = (sk, sv)[c]
            if share < 2:
                ref = ref.at[pl.ds(share * (kv_cols // 2), kv_cols // 2)]
            out.append(ref.at[:, at])
        return out

    def ring(c, way, step, at, dev):
        for ref in refs(c, dev, pieces(step, way)[at]):
            remote(ref, ref, ring_sem.at[0], ring_recv.at[step - 1, at], aims[c, way])

    def settle_ring(step, at):
        first, count, share = pieces(step, 0)[at]
        if share is not None:
            count += kv_cols * rows // q_cols // (2 if step == steps else 1)
        if count:
            settle(sq.at[pl.ds(0, 4 * count)], ring_recv.at[step - 1, at])

    def pass_on(c, dev, item):
        for ref in refs(c, dev, item):
            remote(ref, ref, twin_sem.at[0], twin_sem.at[1], twin)

    def narrow(source, first, dev, to, count):
        def body(i, carry):
            r = pl.ds(pl.multiple_of(first + i * 16, 16), 16)
            out = pl.ds(pl.multiple_of(dev * rows + to + first + i * 16, 16), 16)
            for j in range(tiles):
                col = pl.ds(j * 128, 128)
                sq[out, col] = (source[r, col] * inverse[j:j + 1, :]).astype(jnp.bfloat16)
            return carry

        lax.fori_loop(0, count // 16, body, 0)

    flip = jnp.broadcast_to(inverse[tiles:tiles + 1, :], (128, 128)).T

    def narrow_kv(c, source, dev):
        at = pl.multiple_of(dev * rows, rows)
        for col in range(0, rows, 128):
            (sk, sv)[c][:, pl.ds(pl.multiple_of(at + col, 128), 128)] = (
                source[:, pl.ds(col, 128)] * flip[c * kv_cols:(c + 1) * kv_cols, :]
            ).astype(jnp.bfloat16)

    def origins(c, step):
        back = chip_at(c, lax.rem(spots[c] + chips - step, chips), side) * 2 + core
        return back, chip_at(c, lax.rem(spots[c] + step, chips), side) * 2 + core

    for c in range(2):
        narrow_kv(c, one_kv.at[pl.ds(c * kv_cols, kv_cols)], me)
        narrow(one, c * half, me, 0, half)
        for at in range(PIECES):
            for way in range(2):
                ring(c, way, 1, at, me)
    for c in range(2):
        pass_on(c, me, (0, half, 2))

    for j in range(tiles):
        cq[:, pl.ds(j * 128, 128)] = scale[j:j + 1, :]
    ck[...] = scale[tiles:tiles + 1, 0:kv_cols]
    cv[...] = scale[tiles:tiles + 1, kv_cols:2 * kv_cols]

    for step in range(1, steps + 1):
        devs = {c: origins(c, step) for c in range(2)}
        for at in range(len(pieces(step, 0))):
            if step == 1 and at < len(EARLY):
                count = EARLY[at]
                skip = sum(EARLY[:at])
                for way in range(2):
                    settle(q_in.at[:, pl.ds(0, count)], early_sem.at[at, way])
                    where = skip if way == 0 else ahead - skip - count
                    for c in range(2):
                        narrow(early.at[c, way], where, devs[c][way],
                               c * half + early_rows(way), count)
            settle_ring(step, at)
            for way in range(2):
                item = pieces(step if step > 1 else 0, way)[at]
                for c in range(2):
                    if step < steps:
                        for later, nxt in enumerate(pieces(step + 1, way)):
                            if item[0] <= nxt[0] < item[0] + item[1]:
                                ring(c, way, step + 1, later, devs[c][way])
            for way in range(2):
                item = pieces(step if step > 1 else 0, way)[at]
                for c in range(2):
                    pass_on(c, devs[c][way], item)
    settle(line.at[pl.ds(0, len(row_peers)), lines], stat_sem.at[0])
    settle(column.at[pl.ds(0, len(column_peers)), lines], stat_sem.at[2])
    share = half + kv_cols * rows // q_cols
    settle(sq.at[pl.ds(0, 2 * (chips - 1) * share - 4 * ahead)], ring_sem.at[0])
    settle(q_in.at[:, pl.ds(0, 2 * ahead)], ring_sem.at[1])
    settle(sq.at[pl.ds(0, 2 * chips * share)], twin_sem.at[0])
    settle(sq.at[pl.ds(0, 2 * chips * share)], twin_sem.at[1])


def write_kernel(sq, sk, sv, cq, ck, cv, oq, ok, ov, dq, dk, dv, sem):
    rows = sq.shape[0] // WRITES
    pairs = [(cq, dq), (ck, dk), (cv, dv), (sk, ok), (sv, ov)]
    for n in range(WRITES):
        r = pl.ds(n * rows, rows)
        pairs.append((sq.at[r], oq.at[r]))
    for n, (source, out) in enumerate(pairs):
        pltpu.make_async_copy(source, out, sem.at[min(n, 5)]).start()
    for n, (source, out) in enumerate(pairs[:5] + [(sq, oq)]):
        pltpu.make_async_copy(source, out, sem.at[n]).wait()


def local(ranks, d_model, one_query, other_query, one_key, other_key, one_value, other_value, mix_share, norm_gain):
    rows, q_cols = one_query.shape
    kv_cols = one_key.shape[1]
    whole = ranks * rows
    steps = ranks // 4
    side = math.isqrt(ranks // 2)
    vmem = pl.BlockSpec(memory_space=pltpu.VMEM)
    hbm = pl.BlockSpec(memory_space=pltpu.HBM)
    dma = pltpu.SemaphoreType.DMA
    f32, bf16 = jnp.float32, jnp.bfloat16
    shapes = (
        jax.ShapeDtypeStruct((whole, q_cols), bf16),
        jax.ShapeDtypeStruct((kv_cols, whole), bf16),
        jax.ShapeDtypeStruct((kv_cols, whole), bf16),
        jax.ShapeDtypeStruct((1, q_cols), f32),
        jax.ShapeDtypeStruct((1, kv_cols), f32),
        jax.ShapeDtypeStruct((1, kv_cols), f32),
    )
    landed = pl.pallas_call(
        functools.partial(gather_kernel, ranks, d_model),
        out_shape=tuple(pltpu.VMEM(x.shape, x.dtype) for x in shapes),
        in_specs=[hbm] * 8,
        out_specs=(vmem,) * 6,
        scratch_shapes=[
            pltpu.VMEM((2, 1, rows), f32),
            pltpu.VMEM((2, rows, q_cols), f32),
            pltpu.VMEM((2, 2 * kv_cols, rows), f32),
            pltpu.VMEM((rows, 128), f32),
            pltpu.VMEM((rows, 128), f32),
            pltpu.VMEM((2 * side, 16, 128), f32),
            pltpu.VMEM((side, 16, 128), f32),
            pltpu.VMEM((2, 2, sum(EARLY), q_cols), f32),
            dma((2 + SLABS,)),
            dma((4,)),
            dma((2,)),
            dma((2,)),
            dma((steps, PIECES)),
            dma((2, 2)),
        ],
        compiler_params=pltpu.CompilerParams(
            collective_id=0, has_side_effects=True, vmem_limit_bytes=VMEM_A
        ),
    )(*(
        pltpu.with_memory_space_constraint(x, pltpu.HBM)
        for x in (
            mix_share.reshape(1, rows), norm_gain.reshape(1, rows), one_query, other_query,
            one_key.T, other_key.T, one_value.T, other_value.T,
        )
    ))
    out = pl.pallas_call(
        write_kernel,
        out_shape=shapes,
        in_specs=[vmem] * 6,
        out_specs=(hbm,) * 6,
        scratch_shapes=[dma((6,))],
        compiler_params=pltpu.CompilerParams(vmem_limit_bytes=VMEM_B),
    )(*landed)
    sq, sk, sv, cq, ck, cv = out
    return sq, sk.T, sv.T, cq[0], ck[0], cv[0]


VMEM_A = 10 * 1024 * 1024
VMEM_B = 2 * 1024 * 1024


def solution(mesh):
    def body(one_query, *rest):
        ranks = mesh.shape["rows"]
        return local(ranks, ranks * one_query.shape[0], one_query, *rest)

    return jax.shard_map(
        body,
        mesh=mesh,
        in_specs=(P("rows", "cols"),) * 6 + (P("rows"),) * 2,
        out_specs=(P(None, "cols"),) * 3 + (P("cols"),) * 3,
        check_vma=False,
    )
```

```python
import functools
import math

import jax
import jax.numpy as jnp
from jax import lax
from jax.experimental import pallas as pl
from jax.experimental.pallas import tpu as pltpu
from jax.sharding import PartitionSpec as P

MESH = pl.DeviceIdType.MESH
EARLY = (48, 16)
SLABS = 2
WRITES = 32
STEP_ROWS = 32


def chip_at(cycle, place, side):
    major = lax.div(place, side)
    minor = lax.rem(place - major + side, side)
    y, x = (minor, major) if cycle == 0 else (major, minor)
    return y * side + x


def place_of(cycle, chip, side):
    y, x = lax.div(chip, side), lax.rem(chip, side)
    major, minor = (x, y) if cycle == 0 else (y, x)
    return major * side + lax.rem(minor + major, side)


def gather_kernel(
    ranks, d_model,
    mix_hbm, gain_hbm, oq, tq, ok, tk, ov, tv,
    sq, sk, sv, cq, ck, cv,
    coefs, q_in, kv_in, col_a, col_b, line, column, early,
    load_sem, stat_sem, ring_sem, twin_sem, ring_recv, early_sem,
):
    me = lax.axis_index("rows")
    chips = ranks // 2
    side = math.isqrt(chips)
    steps = chips // 2
    chip, core = lax.div(me, 2), lax.rem(me, 2)
    twin = chip * 2 + 1 - core
    rows, q_cols = oq.shape
    kv_cols = ok.shape[0]
    half = rows // 2
    slab = rows // SLABS
    tiles = q_cols // 128
    one, one_kv = q_in.at[0], kv_in.at[0]

    y, x = lax.div(chip, side), lax.rem(chip, side)
    order = sorted(range(1, side), key=lambda k: -min(k, side - k))
    row_peers = [
        (y * side + lax.rem(x + k, side)) * 2 + n for k in order for n in range(2)
    ] + [twin]
    column_peers = [(lax.rem(y + k, side) * side + x) * 2 + core for k in order]

    barrier = pltpu.get_barrier_semaphore()
    for dev in row_peers + column_peers:
        pl.semaphore_signal(barrier, inc=1, device_id={"rows": dev}, device_id_type=MESH)

    def load(source, held, sem):
        pltpu.make_async_copy(source, held, sem).start()

    def settle(ref, sem):
        pltpu.make_async_copy(ref, ref, sem).wait()

    load(mix_hbm, coefs.at[0], load_sem.at[0])
    load(gain_hbm, coefs.at[1], load_sem.at[0])
    for s in range(SLABS):
        r = pl.ds(s * slab, slab)
        for n, source in enumerate((oq, tq)):
            load(source.at[r], q_in.at[n, r], load_sem.at[2 + s])
    for n, source in enumerate((ok, tk, ov, tv)):
        load(source, kv_in.at[n % 2, pl.ds(n // 2 * kv_cols, kv_cols)], load_sem.at[1])

    settle(coefs, load_sem.at[0])
    a_row = coefs[1] * coefs[0]
    b_row = coefs[1] * (1.0 - coefs[0])
    for c in range(0, rows, 128):
        col_a[pl.ds(c, 128), :] = jnp.broadcast_to(a_row[:, c:c + 128], (128, 128)).T
        col_b[pl.ds(c, 128), :] = jnp.broadcast_to(b_row[:, c:c + 128], (128, 128)).T

    spot = x * 2 + core
    accs = tuple(jnp.zeros((8, 128), jnp.float32) for _ in range(tiles))
    for s in range(SLABS):
        settle(q_in.at[:, pl.ds(s * slab, slab)], load_sem.at[2 + s])

        def body(i, accs):
            r = pl.ds(pl.multiple_of(s * slab + i * STEP_ROWS, STEP_ROWS), STEP_ROWS)
            a, b = col_a[r, :], col_b[r, :]
            new = []
            for j, acc in enumerate(accs):
                c = pl.ds(j * 128, 128)
                f = a * q_in[0, r, c] + b * q_in[1, r, c]
                one[r, c] = f
                new.append(acc + jnp.sum(jnp.abs(f).reshape(STEP_ROWS // 8, 8, 128), axis=0))
            return tuple(new)

        accs = lax.fori_loop(0, slab // STEP_ROWS, body, accs)
    for j, acc in enumerate(accs):
        line[spot, pl.ds(j, 1), :] = jnp.sum(acc, axis=0, keepdims=True)
    settle(kv_in, load_sem.at[1])
    f = a_row * kv_in[0] + b_row * kv_in[1]
    one_kv[...] = f
    sizes = jnp.abs(f)
    size = sizes[:, 0:128]
    for c in range(128, rows, 128):
        size = size + sizes[:, c:c + 128]
    line[spot, pl.ds(tiles, 1), :] = jnp.sum(size.T, axis=0, keepdims=True)

    def remote(src, dst, send, recv, device):
        pltpu.make_async_remote_copy(
            src_ref=src, dst_ref=dst, send_sem=send, recv_sem=recv,
            device_id={"rows": device}, device_id_type=MESH,
        ).start()

    pl.semaphore_wait(barrier, len(row_peers) + len(column_peers))
    lines = pl.ds(0, tiles + 1)
    place = line.at[spot, lines]
    for dev in row_peers:
        remote(place, place, stat_sem.at[0], stat_sem.at[1], dev)

    spots = [place_of(c, chip, side) for c in range(2)]
    aims = {}
    for c in range(2):
        aims[c, 0] = chip_at(c, lax.rem(spots[c] + 1, chips), side) * 2 + core
        aims[c, 1] = chip_at(c, lax.rem(spots[c] + chips - 1, chips), side) * 2 + core

    ahead = sum(EARLY)

    def early_rows(way):
        return 0 if way == 0 else half - ahead

    def send_early(batch):
        skip = sum(EARLY[:batch])
        count = EARLY[batch]
        for c in range(2):
            for way in range(2):
                at = skip if way == 0 else ahead - skip - count
                remote(one.at[pl.ds(c * half + early_rows(way) + at, count)],
                       early.at[c, way, pl.ds(at, count)],
                       ring_sem.at[1], early_sem.at[batch, way], aims[c, way])

    def gathered(ref, peers, sems):
        slots = ref.at[pl.ds(0, peers), lines]
        settle(slots, sems)
        total = ref[0, 0:tiles + 1, :]
        for n in range(1, peers + 1):
            total = total + ref[n, 0:tiles + 1, :]
        return total

    send_early(0)
    column[y, lines, :] = gathered(line, len(row_peers), stat_sem.at[1])
    place = column.at[y, lines]
    for dev in column_peers:
        remote(place, place, stat_sem.at[2], stat_sem.at[3], dev)
    send_early(1)
    total = gathered(column, len(column_peers), stat_sem.at[3])
    scale = total / d_model
    inverse = 1.0 / scale

    def pieces(step, way):
        if step < steps:
            cut = half // 2
            cuts = [(0, cut, 2), (cut, half - cut, None)]
            if step == 1:
                cuts[0] = (ahead, cut - ahead, 2)
        else:
            cut = half // 4
            cuts = [(0, cut, way), (cut, half // 2 - cut, None)]
        if way == 0:
            return cuts
        return [(half - first - count, count, share) for first, count, share in cuts]

    def refs(c, dev, item):
        first, count, share = item
        at = pl.multiple_of(dev * rows + c * half + first, 16)
        out = [sq.at[pl.ds(at, count)]] if count else []
        if share is not None:
            at = pl.ds(pl.multiple_of(dev * rows, rows), rows)
            ref = (sk, sv)[c]
            if share < 2:
                ref = ref.at[pl.ds(share * (kv_cols // 2), kv_cols // 2)]
            out.append(ref.at[:, at])
        return out

    def ring(c, way, step, at, dev):
        for ref in refs(c, dev, pieces(step, way)[at]):
            remote(ref, ref, ring_sem.at[0], ring_recv.at[way, step - 1, at], aims[c, way])

    def settle_ring(way, step, at):
        first, count, share = pieces(step, way)[at]
        extra = 0 if share is None else kv_cols * rows // q_cols // (1 if share == 2 else 2)
        settle(sq.at[pl.ds(0, 2 * (count + extra))], ring_recv.at[way, step - 1, at])

    def pass_on(c, dev, item):
        for ref in refs(c, dev, item):
            remote(ref, ref, twin_sem.at[0], twin_sem.at[1], twin)

    def narrow(source, first, dev, to, count):
        def body(i, carry):
            r = pl.ds(pl.multiple_of(first + i * 16, 16), 16)
            out = pl.ds(pl.multiple_of(dev * rows + to + i * 16, 16), 16)
            for j in range(tiles):
                col = pl.ds(j * 128, 128)
                sq[out, col] = (source[r, col] * inverse[j:j + 1, :]).astype(jnp.bfloat16)
            return carry

        lax.fori_loop(0, count // 16, body, 0)

    flip = jnp.broadcast_to(inverse[tiles:tiles + 1, :], (128, 128)).T

    def narrow_kv(c, source, dev):
        at = pl.multiple_of(dev * rows, rows)
        for col in range(0, rows, 128):
            (sk, sv)[c][:, pl.ds(pl.multiple_of(at + col, 128), 128)] = (
                source[:, pl.ds(col, 128)] * flip[c * kv_cols:(c + 1) * kv_cols, :]
            ).astype(jnp.bfloat16)

    def origins(c, step):
        back = chip_at(c, lax.rem(spots[c] + chips - step, chips), side) * 2 + core
        return back, chip_at(c, lax.rem(spots[c] + step, chips), side) * 2 + core

    for c in range(2):
        narrow_kv(c, one_kv.at[pl.ds(c * kv_cols, kv_cols)], me)
        narrow(one, c * half, me, c * half, half)
        for at in range(2):
            for way in range(2):
                ring(c, way, 1, at, me)
    for step in range(1, steps + 1):
        devs = {c: origins(c, step) for c in range(2)}
        for at in range(2):
            for way in range(2):
                if step == 1 and at == 0:
                    for batch, count in enumerate(EARLY):
                        settle(q_in.at[:, pl.ds(0, count)], early_sem.at[batch, way])
                    for c in range(2):
                        narrow(early.at[c, way], 0, devs[c][way], c * half + early_rows(way), ahead)
                settle_ring(way, step, at)
                item = pieces(min(step, steps) if step > 1 else 0, way)[at]
                for c in range(2):
                    if step < steps:
                        for later, nxt in enumerate(pieces(step + 1, way)):
                            if item[0] <= nxt[0] < item[0] + item[1]:
                                ring(c, way, step + 1, later, devs[c][way])
                for c in range(2):
                    pass_on(c, devs[c][way], item)
        if step > 1:
            continue
        for c in range(2):
            pass_on(c, me, (0, half, 2))

        for j in range(tiles):
            cq[:, pl.ds(j * 128, 128)] = scale[j:j + 1, :]
        ck[...] = scale[tiles:tiles + 1, 0:kv_cols]
        cv[...] = scale[tiles:tiles + 1, kv_cols:2 * kv_cols]
    settle(line.at[pl.ds(0, len(row_peers)), lines], stat_sem.at[0])
    settle(column.at[pl.ds(0, len(column_peers)), lines], stat_sem.at[2])
    share = half + kv_cols * rows // q_cols
    settle(sq.at[pl.ds(0, 2 * (chips - 1) * share - 4 * ahead)], ring_sem.at[0])
    settle(q_in.at[:, pl.ds(0, 2 * ahead)], ring_sem.at[1])
    settle(sq.at[pl.ds(0, 2 * chips * share)], twin_sem.at[0])
    settle(sq.at[pl.ds(0, 2 * chips * share)], twin_sem.at[1])


def write_kernel(sq, sk, sv, cq, ck, cv, oq, ok, ov, dq, dk, dv, sem):
    rows = sq.shape[0] // WRITES
    pairs = [(cq, dq), (ck, dk), (cv, dv), (sk, ok), (sv, ov)]
    for n in range(WRITES):
        r = pl.ds(n * rows, rows)
        pairs.append((sq.at[r], oq.at[r]))
    for n, (source, out) in enumerate(pairs):
        pltpu.make_async_copy(source, out, sem.at[min(n, 5)]).start()
    for n, (source, out) in enumerate(pairs[:5] + [(sq, oq)]):
        pltpu.make_async_copy(source, out, sem.at[n]).wait()


def local(ranks, d_model, one_query, other_query, one_key, other_key, one_value, other_value, mix_share, norm_gain):
    rows, q_cols = one_query.shape
    kv_cols = one_key.shape[1]
    whole = ranks * rows
    steps = ranks // 4
    side = math.isqrt(ranks // 2)
    vmem = pl.BlockSpec(memory_space=pltpu.VMEM)
    hbm = pl.BlockSpec(memory_space=pltpu.HBM)
    dma = pltpu.SemaphoreType.DMA
    f32, bf16 = jnp.float32, jnp.bfloat16
    shapes = (
        jax.ShapeDtypeStruct((whole, q_cols), bf16),
        jax.ShapeDtypeStruct((kv_cols, whole), bf16),
        jax.ShapeDtypeStruct((kv_cols, whole), bf16),
        jax.ShapeDtypeStruct((1, q_cols), f32),
        jax.ShapeDtypeStruct((1, kv_cols), f32),
        jax.ShapeDtypeStruct((1, kv_cols), f32),
    )
    landed = pl.pallas_call(
        functools.partial(gather_kernel, ranks, d_model),
        out_shape=tuple(pltpu.VMEM(x.shape, x.dtype) for x in shapes),
        in_specs=[hbm] * 8,
        out_specs=(vmem,) * 6,
        scratch_shapes=[
            pltpu.VMEM((2, 1, rows), f32),
            pltpu.VMEM((2, rows, q_cols), f32),
            pltpu.VMEM((2, 2 * kv_cols, rows), f32),
            pltpu.VMEM((rows, 128), f32),
            pltpu.VMEM((rows, 128), f32),
            pltpu.VMEM((2 * side, 16, 128), f32),
            pltpu.VMEM((side, 16, 128), f32),
            pltpu.VMEM((2, 2, sum(EARLY), q_cols), f32),
            dma((2 + SLABS,)),
            dma((4,)),
            dma((2,)),
            dma((2,)),
            dma((2, steps, 2)),
            dma((2, 2)),
        ],
        compiler_params=pltpu.CompilerParams(
            collective_id=0, has_side_effects=True, vmem_limit_bytes=VMEM_A
        ),
    )(*(
        pltpu.with_memory_space_constraint(x, pltpu.HBM)
        for x in (
            mix_share.reshape(1, rows), norm_gain.reshape(1, rows), one_query, other_query,
            one_key.T, other_key.T, one_value.T, other_value.T,
        )
    ))
    out = pl.pallas_call(
        write_kernel,
        out_shape=shapes,
        in_specs=[vmem] * 6,
        out_specs=(hbm,) * 6,
        scratch_shapes=[dma((6,))],
        compiler_params=pltpu.CompilerParams(vmem_limit_bytes=VMEM_B),
    )(*landed)
    sq, sk, sv, cq, ck, cv = out
    return sq, sk.T, sv.T, cq[0], ck[0], cv[0]


VMEM_A = 10 * 1024 * 1024
VMEM_B = 2 * 1024 * 1024


def solution(mesh):
    def body(one_query, *rest):
        ranks = mesh.shape["rows"]
        return local(ranks, ranks * one_query.shape[0], one_query, *rest)

    return jax.shard_map(
        body,
        mesh=mesh,
        in_specs=(P("rows", "cols"),) * 6 + (P("rows"),) * 2,
        out_specs=(P(None, "cols"),) * 3 + (P("cols"),) * 3,
        check_vma=False,
    )
```
